8 devices in a mesh: rep: 1 (over z), dp: 8 (over x, y, core).
Axes of the slice: x: 2, y: 2, z: 1, core: 2. Of those that a mesh axis runs over, the one named last changes fastest.
Arguments:
- x: bfloat16 [8, 2048, 1536], P(('rep', 'dp'))
- dy: bfloat16 [8, 2048, 1536], P(('rep', 'dp'))
- w_gate: bfloat16 [2, 1536, 4224], P(None, 'dp')
- w_up: bfloat16 [2, 1536, 4224], P(None, 'dp')
- w_down: bfloat16 [2, 4224, 1536], P(None, 'dp')
- m_w_gate: float32 [2, 1536, 4224], P(None, 'dp')
- m_w_up: float32 [2, 1536, 4224], P(None, 'dp')
- m_w_down: float32 [2, 4224, 1536], P(None, 'dp')
- v_w_gate: float32 [2, 1536, 4224], P(None, 'dp')
- v_w_up: float32 [2, 1536, 4224], P(None, 'dp')
- v_w_down: float32 [2, 4224, 1536], P(None, 'dp')
Outputs:
- output 1: bfloat16 [2, 1536, 4224], P('rep', 'dp')
- output 2: bfloat16 [2, 1536, 4224], P('rep', 'dp')
- output 3: bfloat16 [2, 4224, 1536], P('rep', 'dp')
- output 4: float32 [2, 1536, 4224], P('rep', 'dp')
- output 5: float32 [2, 1536, 4224], P('rep', 'dp')
- output 6: float32 [2, 4224, 1536], P('rep', 'dp')
- output 7: float32 [2, 1536, 4224], P('rep', 'dp')
- output 8: float32 [2, 1536, 4224], P('rep', 'dp')
- output 9: float32 [2, 4224, 1536], P('rep', 'dp')
All inputs are finite; a program needn't handle non-finite values.
Results may differ from the reference program's by a relative error of at most 0.022.
Values are sent between devices in bfloat16 or wider.
A program may use at most 2 GiB of HBM per device.

```python
import jax
import jax.numpy as jnp
from jax import lax

SEQUENCES = 8
TOKENS = 2048
D = 1536
FF = 4224
LAYERS = 2
NAMES = ("w_gate", "w_up", "w_down")
SHAPES = {"w_gate": (LAYERS, D, FF), "w_up": (LAYERS, D, FF), "w_down": (LAYERS, FF, D)}


def bump(key, n, height):
    away = (jnp.arange(n, dtype=jnp.int32) - jax.random.randint(key, (), 0, n, jnp.int32)) % n
    return jnp.where(away < n // 8, height, 1.0)


def together(key, own, strength):
    shared = jax.random.normal(key, own.shape[1:], jnp.float32)
    return (own + strength * shared) * lax.rsqrt(1 + strength * strength)


def setup_inputs(seed: int = 0, part: int = 0) -> dict:
    kx, kdy, ka, kb, kz, kf, kh, kl, *keys = jax.random.split(jax.random.key(seed), 8 + 3 * len(NAMES))
    kx, kdy, ka, kb = (jax.random.fold_in(k, part) for k in (kx, kdy, ka, kb))
    kw, km, kv = (keys[i::3] for i in range(3))
    shape = (SEQUENCES, TOKENS, D)
    much_x, much_dy = jax.random.uniform(kz, (2,), jnp.float32, 0.0, 1.0)
    loud = 2.0 ** jax.random.uniform(jax.random.fold_in(kz, 1), (), jnp.float32, -1.0, 2.0)
    layers = 2.0 ** jax.random.uniform(kl, (LAYERS, 1, 1), jnp.float32, -1.0, 1.0)
    x = together(ka, jax.random.normal(kx, shape, jnp.float32), much_x) * bump(kf, D, 4.0)
    dy = together(kb, jax.random.normal(kdy, shape, jnp.float32), much_dy)
    drawn = {"x": x.astype(jnp.bfloat16), "dy": (loud * dy * (SEQUENCES * TOKENS) ** -0.5).astype(jnp.bfloat16)}
    for key, name in zip(kw, NAMES, strict=True):
        w = jax.random.normal(key, SHAPES[name], jnp.float32) * SHAPES[name][1] ** -0.5
        drawn[name] = (w * {"w_gate": 1.0, "w_up": bump(kh, FF, 4.0), "w_down": layers}[name]).astype(jnp.bfloat16)
    for key, name in zip(km, NAMES, strict=True):
        drawn[f"m_{name}"] = 0.1 * jax.random.normal(key, SHAPES[name], jnp.float32)
    for key, name in zip(kv, NAMES, strict=True):
        drawn[f"v_{name}"] = jax.random.uniform(key, SHAPES[name], jnp.float32, 0.005, 0.015)
    return drawn


def matmul(a, w):
    return jnp.dot(a, w, preferred_element_type=jnp.float32).astype(jnp.bfloat16)


def normed(h):
    wide = h.astype(jnp.float32)
    scale = lax.rsqrt(jnp.mean(wide**2, -1, keepdims=True) + 1e-6)
    return (wide * scale).astype(jnp.bfloat16)


def layer(h, w):
    a = normed(h)
    gate = jnp.dot(a, w["w_gate"], preferred_element_type=jnp.float32)
    up = jnp.dot(a, w["w_up"], preferred_element_type=jnp.float32)
    return h + matmul((jax.nn.silu(gate) * up).astype(jnp.bfloat16), w["w_down"])


def adamw(w, m, v, g):
    m = 0.9 * m + 0.1 * g
    v = 0.95 * v + 0.05 * g * g
    step = m * lax.rsqrt(v + 1e-8) + 0.1 * w
    return (w - 0.02 * step).astype(jnp.bfloat16), m, v


def clipped(gradients, sum_of_squares, count):
    factor = jnp.minimum(1.0, 0.5 * lax.rsqrt(sum_of_squares / count + 1e-30))
    return [g * factor for g in gradients]


def stack(weights, h):
    return lax.scan(lambda h, w: (layer(h, w), None), h, weights)[0]


def reference(x, dy, w_gate, w_up, w_down, m_w_gate, m_w_up, m_w_down, v_w_gate, v_w_up, v_w_down):
    weights = dict(zip(NAMES, (w_gate, w_up, w_down), strict=True))

    def take(so_far, sequence):
        h, by_y = sequence
        _, back = jax.vjp(lambda w: stack(w, h), weights)
        return jax.tree.map(lambda total, term: total + term.astype(jnp.float32), so_far, back(by_y)[0]), None

    none_yet = {name: jnp.zeros(w.shape, jnp.float32) for name, w in weights.items()}
    by_weights, _ = lax.scan(take, none_yet, (x, dy))
    gradients = [by_weights[name].astype(jnp.bfloat16).astype(jnp.float32) for name in NAMES]
    gradients = clipped(gradients, sum(jnp.sum(g * g) for g in gradients), sum(g.size for g in gradients))
    new = [
        adamw(w.astype(jnp.float32), m, v, g)
        for w, m, v, g in zip((w_gate, w_up, w_down), (m_w_gate, m_w_up, m_w_down), (v_w_gate, v_w_up, v_w_down), gradients, strict=True)
    ]
    return tuple(one[which] for which in range(3) for one in new)
```

```python
import functools
import jax
import jax.numpy as jnp
from jax import lax
from jax.experimental import pallas as pl
from jax.experimental.pallas import tpu as pltpu
from jax.sharding import PartitionSpec as P

BF, F32 = jnp.bfloat16, jnp.float32
MESH = pl.DeviceIdType.MESH
T, D, FF = 2048, 1536, 4224
RG, RD = 192, 528
COL, WIDE, LAST = 256, 512, 128
TALL, HALF, MAIN = 1024, 768, 4096
NC = MAIN // COL
RDC, ND, PER = 176, 9, 26
Q, RING = 2 * PER, 12
DOWN, BOTH, TAIL = (RDC, WIDE), (RG, WIDE), (RG, COL)
OX, OY, OS, FX, FY, SX, SY, SD = range(8)
UNITS = ((0, (0, 8)), (0, (8, NC)), (0, None), (1, (0, 8)), (1, (8, 12)), (1, (12, NC)), (1, None))
YES, NO = True, False
S2, S3, S4 = 2, 3, 4
PAIR = (0, 1)


def cut(i, n):
    return pl.ds(i * n, n) if isinstance(i, int) else pl.ds(pl.multiple_of(i * n, n), n)


def block(i, n):
    return pl.ds(pl.multiple_of(i, 8), n)


def start(copies):
    for c in copies:
        c.start()


def wait(copies):
    for c in copies:
        c.wait()


def when(condition, do):
    if isinstance(condition, bool):
        if condition:
            do()
    else:
        pl.when(condition)(do)


def local(src, dst, sem):
    return pltpu.make_async_copy(src, dst, sem)


def dot(a, b, nt=NO):
    return lax.dot_general(a, b, (((1,), (int(nt),)), ((), ())), preferred_element_type=F32)


def gated(gate, up):
    s = jax.nn.sigmoid(gate)
    silu = gate * s
    return up * (s + silu * (1.0 - s)), silu, (silu * up).astype(BF)


def kernel(x, dy, wg, wu, wd, gg, gu, gd, squares, WG, WU, WD, aT, hT, R, Rt, h1, own, inx, iny, DG, DU,
           A, Y, dgi, d2r, sq, send, recv, keeps, dgi_sem, in_sem, out_sem, d2r_sem, d2s_sem, own_sem, sq_send, sq_recv, ld, ldl, st, credit, room):
    me = lax.axis_index("dp")
    core, y_, x_ = me % S2, (me // 2) % S2, me // 4
    at = lambda a, b, c: (a * 2 + b) * 2 + c
    xn, yn, dg, sib = at(1 - x_, y_, core), at(x_, 1 - y_, core), at(1 - x_, 1 - y_, core), at(x_, y_, 1 - core)
    other = lambda dev: dev + 1 - 2 * (dev % S2)
    everyone = [(me + k) % 8 for k in range(1, 8)]
    order = [other(dg), other(xn), other(yn), sib, dg, xn, yn, me]

    def remote(src, dst, sender, receiver, to):
        return pltpu.make_async_remote_copy(src, dst, sender, receiver, device_id={"dp": to}, device_id_type=MESH)

    def signal(sem, to):
        pl.semaphore_signal(sem, inc=1, device_id={"dp": to}, device_id_type=MESH)

    barrier = pltpu.get_barrier_semaphore()
    for dev in everyone:
        signal(barrier, dev)
    pl.semaphore_wait(barrier, len(everyone))

    to_whom = (xn, yn, sib, xn, yn, sib, sib, sib)
    whose = (me, me, me, yn, xn, xn, yn, dg)

    def half(u, p, dev):
        l, blocks = UNITS[u]
        refs = (wg, wu, wd) if dev is None else (WG, WU, WD)
        ref, height, rows, top, cols = refs[2], RD, RD // 2, p * (RD // 2), pl.ds(0, D)
        if blocks:
            lo, hi = blocks[0] * COL, FF if blocks[1] == NC else blocks[1] * COL
            ref, height, rows, top, cols = refs[p], RG, RG, 0, pl.ds(lo, hi - lo)
        if dev is not None:
            top = pl.multiple_of(dev * height + top, 8)
        return ref.at[l, pl.ds(top, rows), cols]

    def hop(u, k, p):
        src = half(u, p, None if k <= OS else whose[k])
        return remote(src, half(u, p, whose[k]), send.at[u, k, p], recv.at[u, k, p], to_whom[k])

    def keep(u):
        return [local(half(u, p, None), half(u, p, me), keeps.at[u, p]) for p in PAIR]

    def first(u):
        start(hop(u, k, p) for k, p in ((OX, 0), (OY, 1), (OX, 1), (OY, 0), (OS, 0), (OS, 1)))

    def arrived(u, *which):
        for k, p in which:
            hop(u, k, p).wait_recv()

    def point1(u):
        arrived(u, (OX, 0), (OY, 1))
        start([hop(u, FY, 0), hop(u, FX, 1)])
        if u + 1 < len(UNITS):
            first(u + 1)
        start([hop(u, SX, 0), hop(u, SY, 1)])

    def point2(u):
        arrived(u, (OX, 1), (OY, 0))
        start([hop(u, SX, 1), hop(u, SY, 0)])

    def point3(u):
        arrived(u, (FY, 0), (FX, 1))
        start(hop(u, SD, p) for p in PAIR)

    def point4(u):
        arrived(u, *((k, p) for k in (OS, SX, SY, SD) for p in PAIR))
        wait(keep(u))

    def rest(u):
        point2(u)
        point3(u)
        point4(u)

    def norm():
        @pl.loop(0, T // COL)
        def _(i):
            rows = cut(i, COL)
            wide = A[rows, :].astype(F32)
            scale = lax.rsqrt(jnp.mean(wide * wide, -1, keepdims=YES) + 1e-6)
            A[rows, :] = (wide * scale).astype(BF)

    def forward(H, hTs):
        def put_T(l, c, what):
            return local(hTs.at[c % S2], what.at[l, cut(c, COL), :], st.at[c % S2, 0])

        def transposed(l):
            n = D // COL

            @pl.loop(0, n)
            def _(c):
                pl.when(c >= 2)(lambda: put_T(l, c - 2, aT).wait())
                hTs[c % S2] = A[:, cut(c, COL)].T
                put_T(l, c, aT).start()

            wait(put_T(l, c, aT) for c in (n - 2, n - 1))

        def gate_up(u, points, Wb, r32):
            l, (lo, end) = UNITS[u]
            n = end - lo
            hi = end == NC

            def get(j):
                return [local(W.at[l, :, cut(j, COL)], Wb.at[j % S3, :, cut(i, COL)], ld.at[j % S3, i]) for i, W in enumerate((WG, WU))]

            def put(j):
                return [local(r32.at[j % S2], R.at[l, j], st.at[j % S2, 1]), put_T(l, j, hT)]

            def work(j, w, k, out):
                @pl.loop(0, 2)
                def _(i):
                    rows = cut(i, TALL)
                    r = dot(A[rows, :], Wb[k, :, pl.ds(0, 2 * w)])
                    by_gate, by_up, hid = gated(r[:, :w], r[:, w:])
                    r32[out, rows, pl.ds(0, w)] = by_gate
                    r32[out, rows, pl.ds(w, w)] = by_up
                    if l == 0:
                        H[rows, pl.ds(MAIN, w) if w == LAST else cut(j, COL)] = hid
                    hTs[out, pl.ds(0, w), rows] = hid.T

            ws = [local(W.at[l, :, pl.ds(MAIN, LAST)], Wb.at[NC % S3, :, cut(i, LAST)], ld.at[NC % S3, i]) for i, W in enumerate((WG, WU))]
            start(get(lo) + get(lo + 1))

            @pl.loop(lo, lo + n)
            def _(j):
                wait(get(j))
                pl.when(j + 2 < lo + n)(lambda: start(get(j + 2)))
                pl.when(j >= lo + 2)(lambda: wait(put(j - 2)))
                work(j, COL, j % S3, j % S2)
                start(put(j))
                if hi:
                    pl.when(j == NC - 2)(lambda: start(ws))
                for i, (do, unit) in points:
                    pl.when(j == lo + i)(lambda: do(unit))

            wait(put(lo + n - 2))
            if hi:
                wait(ws)
                work(NC, LAST, NC % S3, 0)
                outs = [local(r32.at[0, :, pl.ds(0, COL)], Rt.at[l], st.at[0, 1]), local(hTs.at[0, pl.ds(0, LAST)], hT.at[l, pl.ds(MAIN, LAST), :], st.at[0, 0])]
                start(outs)
                wait(outs)
            wait(put(lo + n - 1))

        def both(units, *points):
            def body(Wb, r32):
                for u, due in zip(units, points):
                    gate_up(u, due, Wb, r32)
                    if u < units[-1]:
                        late = [do for _, (do, unit) in due if unit == u + 1]
                        for do in (point1, point2, point3, point4):
                            if do not in late:
                                do(u + 1)

            pl.run_scoped(body, pltpu.VMEM((S3, D, WIDE), BF), pltpu.VMEM((S2, T, WIDE), F32))

        def down(Wd, xs):
            n = D // COL

            def get(c):
                return [local(WD.at[0, :, cut(c, COL)], Wd.at[c % S2], ld.at[c % S2, 0]), local(x.at[:, cut(c, COL)], xs.at[c % S2], ld.at[c % S2, 1])]

            start(get(0))

            @pl.loop(0, n)
            def _(c):
                wait(get(c))
                pl.when(c + 1 < n)(lambda: start(get(c + 1)))

                @pl.loop(0, 2)
                def _(i):
                    rows = cut(i, TALL)
                    r = dot(H[rows, :], Wd[c % S2]).astype(BF)
                    A[rows, cut(c, COL)] = (xs[c % S2, rows, :].astype(F32) + r.astype(F32)).astype(BF)

                pl.when(c == 3)(lambda: point1(3))

        load = local(x, A, ld.at[0, 0])
        load.start()
        load.wait()
        norm()
        transposed(0)
        point1(0)
        rest(0)
        both((0, 1), [(5, (point1, 1))], [(5, (point1, 2))])
        rest(2)
        pl.run_scoped(down, pltpu.VMEM((S2, FF, COL), BF), pltpu.VMEM((S2, T, COL), BF))
        save = local(A, h1, ld.at[0, 0])
        save.start()
        save.wait()
        norm()
        transposed(1)
        rest(3)
        both((3, 4, 5), [(1, (point1, 4)), (3, (point2, 4)), (5, (point3, 4))], [(0, (point1, 5)), (2, (point2, 5))], [(2, (point1, 6))])

    first(0)
    by_y = local(dy, Y, st.at[3, 0])
    by_y.start()
    for u in range(len(UNITS)):
        start(keep(u))
    pl.run_scoped(forward, pltpu.VMEM((T, FF), BF), pltpu.VMEM((S2, COL, T), BF))

    def backward(sl, pend, d2s, ow):
        def d2d(q, kind):
            r, n = kind
            rows, cols = pl.ds(0, 4 * r), pl.ds(0, n)
            return remote(d2s.at[q % S2, rows, cols], d2r.at[q % S3, rows, cols], d2s_sem.at[q % S2], d2r_sem.at[q % S3], sib)

        def halves(kind):
            r, n = kind
            return pl.ds(0, r), pl.ds(0, n // 2), pl.ds(n // 2, n // 2)

        def outs(q, kind):
            s = q % RING
            rows, lo, hi = halves(kind)
            a, b, c = sl.at[s, 0], sl.at[s, 1], sl.at[s, 2]
            ends = [(a.at[rows, lo], dgi.at[s, 0, rows, lo], dgi_sem.at[s, 0], xn), (a.at[rows, hi], dgi.at[s, 1, rows, lo], dgi_sem.at[s, 1], yn)]
            ends += [(b.at[rows, lo], inx.at[q, rows, lo], in_sem.at[q, 0], xn), (c.at[rows, hi], iny.at[q, rows, hi], in_sem.at[q, 1], yn)]
            ends += [(b.at[rows, hi], inx.at[q, rows, hi], in_sem.at[q, 2], xn), (c.at[rows, lo], iny.at[q, rows, lo], in_sem.at[q, 3], yn)]
            return [remote(src, dst, out_sem.at[s, i], sem, to) for i, (src, dst, sem, to) in enumerate(ends)]

        def by_kind(q, do):
            c = q % PER
            pl.when(c < ND)(lambda: do(q, DOWN))
            pl.when(jnp.logical_and(c >= ND, c < PER - 1))(lambda: do(q, BOTH))
            pl.when(c == PER - 1)(lambda: do(q, TAIL))

        def release(q, kind):
            for c in outs(q, kind):
                c.wait_send()

        def put_own(q, kind):
            r, n = kind
            return local(ow.at[q % S2, pl.ds(0, r), pl.ds(0, n)], own.at[q, pl.ds(0, r), pl.ds(0, n)], own_sem.at[q % S2])

        def wait_own(q, kind):
            put_own(q, kind).wait()

        def before_add(q, kind):
            when(q >= RING, lambda: by_kind(jnp.int32(q - RING), release))
            c = d2d(q, kind)
            c.wait_recv()
            c.wait_send()
            when(q >= 2, lambda: by_kind(jnp.int32(q - 2), wait_own))

        def sums(q, kind, lhs, rhs):
            r, n = kind
            h, s = n // 2, q % RING
            rows, lo, hi = halves(kind)
            t = dot(lhs[pl.ds(4 * r, 4 * r), :], rhs) + d2r[q % S3, pl.ds(0, 4 * r), pl.ds(0, n)].astype(F32)
            sl[s, 0, rows, pl.ds(0, n)] = t[:r].astype(BF)
            sl[s, 1, rows, lo] = t[r : 2 * r, :h].astype(BF)
            pend[s, 1, rows, lo] = t[r : 2 * r, h:]
            sl[s, 2, rows, hi] = t[2 * r : 3 * r, h:].astype(BF)
            pend[s, 0, rows, lo] = t[2 * r : 3 * r, :h]
            ow[q % S2, rows, pl.ds(0, n)] = t[3 * r :]

        def theirs(q, kind, lhs, rhs):
            r, n = kind
            d2s[q % S2, pl.ds(0, 4 * r), pl.ds(0, n)] = dot(lhs[pl.ds(0, 4 * r), :], rhs).astype(BF)

        def after_add(q, kind):
            def room_there():
                for i in PAIR:
                    pl.semaphore_wait(room.at[i], 1)

            when(q >= RING, room_there)
            start(outs(q, kind)[:4])
            put_own(q, kind).start()
            when(q < Q - 3, lambda: signal(credit, sib))

        def send_d2d(q, kind):
            when(q >= 3, lambda: pl.semaphore_wait(credit, 1))
            d2d(q, kind).start()

        def serve(q, kind):
            s = q % RING
            rows, lo, hi = halves(kind)
            o = outs(q, kind)
            for c in o[:2]:
                c.wait_recv()
            sl[s, 2, rows, lo] = (pend[s, 0, rows, lo] + dgi[s, 0, rows, lo].astype(F32)).astype(BF)
            sl[s, 1, rows, hi] = (pend[s, 1, rows, lo] + dgi[s, 1, rows, lo].astype(F32)).astype(BF)
            start(o[4:])

            def done():
                for i, dev in enumerate((xn, yn)):
                    signal(room.at[i], dev)

            when(q < Q - RING, done)

        def serve_some(i, steps, lo, count, kind):
            a, b = (i * count) // steps, ((i + 1) * count) // steps
            pl.when(jnp.logical_and(b > a, jnp.logical_and(i >= 0, i < steps)))(lambda: serve(lo + a, kind))

        def down_gradient(base, l, then):
            def body(L):
                def get(t):
                    return [local(hT.at[l, block(dev * RD + t * RDC, RDC), :], L.at[t % S2, cut(b, RDC), :], ldl.at[t % S2, b]) for b, dev in enumerate(order)]

                def one(c, do_s, do_m):
                    q, e = base + c, c - 2
                    if do_s:
                        pl.when(c % S3 == 0)(lambda: wait(get(c // 3)))
                        pl.when(jnp.logical_and(c % S3 == 2, c < ND - 1))(lambda: start(get(c // 3 + 1)))
                    if do_m:
                        before_add(q - 2, DOWN)
                        sums(q - 2, DOWN, L.at[(e // 3) % S2], Y[:, cut(e % S3, WIDE)])
                    if do_s:
                        theirs(q, DOWN, L.at[(c // 3) % S2], Y[:, cut(c % S3, WIDE)])
                        send_d2d(q, DOWN)
                    if do_m:
                        after_add(q - 2, DOWN)

                start(get(0))
                @pl.loop(0, 2)
                def _(c):
                    one(c, YES, NO)

                @pl.loop(2, ND)
                def _(c):
                    one(c, YES, YES)
                    if l == 1:
                        pl.when(c == 2)(lambda: point2(6))
                        pl.when(c == 7)(lambda: point3(6))
                    else:
                        serve_some(c - 5, S4, base, S3, DOWN)

                then()

                @pl.loop(ND, ND + 2)
                def _(c):
                    one(c, NO, YES)

            pl.run_scoped(body, pltpu.VMEM((S2, 8 * RDC, T), BF))

        def layer_gradients(base, l):
            g = base + ND

            def outer(Wd, Rb, dgu):
                lhs = lambda L: [local(aT.at[l, block(dev * RG, RG), :], L.at[cut(b, RG), :], ldl.at[2, b]) for b, dev in enumerate(order)]
                is_last = lambda c: isinstance(c, int) and c == NC
                kind = lambda c: TAIL if is_last(c) else BOTH
                part = lambda c: dgu[c % S4, :, pl.ds(0, kind(c)[1])]

                def get(c):
                    k = c % S2
                    if is_last(c):
                        return [local(WD.at[l, pl.ds(MAIN, LAST), :], Wd.at[k, pl.ds(0, LAST), :], ld.at[k, 0]), local(Rt.at[l], Rb.at[k, :, pl.ds(0, COL)], ld.at[k, 1])]
                    return [local(WD.at[l, cut(c, COL), :], Wd.at[k], ld.at[k, 0]), local(R.at[l, c], Rb.at[k], ld.at[k, 1])]

                def put(c):
                    w, cols = (LAST, pl.ds(MAIN, LAST)) if is_last(c) else (COL, cut(c, COL))
                    return [local(dgu.at[c % S4, :, cut(i, w)], W.at[:, cols], st.at[c % S4, i]) for i, W in enumerate((DG, DU))]

                def step(s, L, do_f, do_s, do_m):
                    c, e = s - 1, s - 3
                    if do_f:
                        wait(get(s))
                        when(jnp.logical_and(s > 0, s < NC - 1) if not isinstance(s, int) else 0 < s < NC - 1, lambda: start(get(s + 1)))
                        if l == 1:
                            when(s >= 4, lambda: wait(put(s - 4)))
                    if do_m:
                        before_add(g + e, kind(e))
                        sums(g + e, kind(e), L, part(e))
                    if do_s:
                        theirs(g + c, kind(c), L, part(c))
                    if do_f:
                        w = LAST if is_last(s) else COL
                        d = dot(Y[...], Wd[s % S2, pl.ds(0, w), :], nt=YES).astype(BF).astype(F32)
                        for i in PAIR:
                            dgu[s % S4, :, cut(i, w)] = (d * Rb[s % S2, :, cut(i, w)]).astype(BF)
                    if do_s:
                        send_d2d(g + c, kind(c))
                    if do_f and l == 1:
                        start(put(s))
                    if do_m:
                        after_add(g + e, kind(e))

                def down_served(s):
                    if l == 1:
                        serve_some(2 * s, 12, base, ND, DOWN)
                        serve_some(2 * s + 1, 12, base, ND, DOWN)
                    else:
                        serve_some(s, ND - S3, base + S3, ND - S3, DOWN)

                def ahead():
                    if l == 1:
                        point4(6)
                    start(get(0) + get(1))

                def body(L):
                    start(lhs(L))
                    step(0, L, YES, NO, NO)
                    down_served(jnp.int32(0))
                    wait(lhs(L))

                    @pl.loop(1, 3)
                    def _(s):
                        step(s, L, YES, YES, NO)
                        down_served(s)

                    @pl.loop(3, NC)
                    def _(s):
                        step(s, L, YES, YES, YES)
                        pl.when(s == NC - 2)(lambda: start(get(NC)))
                        down_served(s)
                        serve_some(s - 6, 11, g, 10, BOTH)

                    step(NC, L, YES, YES, YES)
                    serve(g + 9, BOTH)
                    step(NC + 1, L, NO, YES, YES)
                    step(NC + 2, L, NO, NO, YES)
                    step(NC + 3, L, NO, NO, YES)
                    if l == 1:
                        for c in range(NC - 3, NC + 1):
                            wait(put(c))

                down_gradient(base, l, ahead)
                pl.run_scoped(body, pltpu.VMEM((D, T), BF))

            V = pltpu.VMEM
            pl.run_scoped(outer, V((S2, COL, D), BF), V((S2, T, WIDE), F32), V((S4, T, WIDE), BF))

        def input_gradient():
            m, n = T // WIDE, D // HALF
            steps = m * n

            def body(W, X, hb):
                def get_x(i, src):
                    return [local(src.at[cut(i % m * 4 + k, LAST), :], X.at[i % S2, cut(k, LAST), :], ldl.at[i % S2, k]) for k in range(4)]

                def get_w(k, src):
                    return local(src.at[1, cut(k % n, HALF), :], W.at[k % S2], ld.at[k % S2, 1])

                get_w(0, WG).start()
                start(get_x(0, DG))
                for up, (grad, weight) in enumerate(((DG, WG), (DU, WU))):
                    @pl.loop(0, steps)
                    def _(i):
                        k = n * up + i // m

                        @pl.when(i % m == 0)
                        def _():
                            get_w(k, weight).wait()
                            pl.when(i < steps - m)(lambda: get_w(k + 1, weight).start())
                            if not up:
                                pl.when(i == steps - m)(lambda: get_w(n, WU).start())

                        wait(get_x(i, grad))
                        pl.when(i < steps - 1)(lambda: start(get_x(i + 1, grad)))
                        if not up:
                            pl.when(i == steps - 1)(lambda: start(get_x(0, DU)))
                        r = dot(X[i % S2], W[k % S2], nt=YES).astype(BF)
                        place = (cut(i % m, WIDE), cut(i // m, HALF))
                        A[place] = (A[place].astype(F32) + r.astype(F32)).astype(BF) if up else r
                        serve_some(steps * up + i, 11, ND + 10, 6, BOTH)

                get_h = lambda i: local(h1.at[cut(i, COL), :], hb.at[i % S2], st.at[i % S2, 0])
                get_h(0).start()
                serve(PER - 1, TAIL)

                @pl.loop(0, T // COL)
                def _(i):
                    get_h(i).wait()
                    pl.when(i < T // COL - 1)(lambda: get_h(i + 1).start())
                    rows = cut(i, COL)
                    f, b = hb[i % S2].astype(F32), A[rows, :].astype(F32)
                    ms = jnp.mean(f * f, -1, keepdims=YES) + 1e-6
                    scale = lax.rsqrt(ms)
                    c = jnp.sum(f * b, -1, keepdims=YES) * (-0.5 * (scale / ms)) * (1.0 / D)
                    back = (b * scale + c * (2.0 * f)).astype(BF)
                    Y[rows, :] = (Y[rows, :].astype(F32) + back.astype(F32)).astype(BF)

            V = pltpu.VMEM
            pl.run_scoped(body, V((S2, HALF, FF), BF), V((S2, WIDE, FF), BF), V((S2, COL, D), BF))

        by_y.wait()
        layer_gradients(0, 1)
        input_gradient()
        layer_gradients(PER, 0)

        for q in (Q - 2, Q - 1):
            by_kind(jnp.int32(q), wait_own)

        def finish(ob, ib, gb, acc):
            def get(q):
                return [local(own.at[q], ob.at[q % S3], ldl.at[q % S3, 0])] + [local(src.at[q], ib.at[q % S3, i], ldl.at[q % S3, i + 1]) for i, src in enumerate((inx, iny))]

            def fetch(q):
                def all_in(q, kind):
                    for c in outs(q, kind)[2:]:
                        c.wait_recv()

                by_kind(q, all_in)
                start(get(q))

            def put(q, kind):
                l, c, s = 1 - q // PER, q % PER, q % S2
                if kind == DOWN:
                    return [local(gb.at[s, pl.ds(0, RDC), :], gd.at[l, cut(c // 3, RDC), cut(c % S3, WIDE)], st.at[s, 0])]
                w = LAST if kind == TAIL else COL
                cols = pl.ds(MAIN, LAST) if kind == TAIL else cut(c - ND, COL)
                return [local(gb.at[s, :, cut(i, w)], dst.at[l, :, cols], st.at[s, i]) for i, dst in enumerate((gg, gu))]

            def one(q):
                pl.when(q < Q - 2)(lambda: fetch(q + 2))
                pl.when(q >= 2)(lambda: by_kind(q - 2, lambda q, kind: wait(put(q, kind))))
                wait(get(q))
                c, s = q % PER, q % S3
                height, width = jnp.where(c < ND, RDC, RG), jnp.where(c == PER - 1, COL, WIDE)
                inside = jnp.logical_and(lax.broadcasted_iota(jnp.int32, (RG, WIDE), 0) < height, lax.broadcasted_iota(jnp.int32, (RG, WIDE), 1) < width)
                g = (ob[s] + ib[s, 0].astype(F32) + ib[s, 1].astype(F32)).astype(BF)
                gb[q % S2] = g
                g = jnp.where(inside, g.astype(F32), 0.0)
                acc[...] += jnp.sum((g * g).reshape(RG // 8, 8, WIDE), 0)
                by_kind(q, lambda q, kind: start(put(q, kind)))

            acc[...] = jnp.zeros_like(acc)
            n = 7
            left = Q - n
            fetch(jnp.int32(0))
            fetch(jnp.int32(1))

            @pl.loop(0, n * (Q - left))
            def _(q):
                pl.when(q % n == 0)(lambda: by_kind(left + q // n, serve))
                one(q)

            @pl.loop(n * (Q - left), Q)
            def _(q):
                one(q)

            for q in (Q - 2, Q - 1):
                by_kind(jnp.int32(q), lambda q, kind: wait(put(q, kind)))
            sq[me] = sum(acc[:, cut(i, LAST)] for i in range(WIDE // LAST))

        V = pltpu.VMEM
        pl.run_scoped(finish, V((S3, RG, WIDE), F32), V((S3, 2, RG, WIDE), BF), V((S2, RG, WIDE), BF), V((8, WIDE), F32))
        tell = [remote(sq.at[me], sq.at[me], sq_send.at[k], sq_recv.at[k], dev) for k, dev in enumerate(everyone)]
        start(tell)
        @pl.loop(Q - RING, Q)
        def _(q):
            by_kind(q, release)

        for u in range(len(UNITS)):
            for k in range(8):
                for p in ((1,) if k == FX else (0,) if k == FY else (0, 1)):
                    hop(u, k, p).wait_send()
        wait(tell)
        sq[0] = sum(sq[i] for i in range(8))
        out = local(sq.at[0], squares, ld.at[0, 0])
        out.start()
        out.wait()

    V = pltpu.VMEM
    pl.run_scoped(backward, V((RING, 3, RG, WIDE), BF), V((RING, 2, RG, COL), F32), V((S2, 4 * RG, WIDE), BF), V((S2, RG, WIDE), F32))


def gradients_of(x, dy, wg, wu, wd):
    S, V = jax.ShapeDtypeStruct, pltpu.VMEM
    dma, regular = pltpu.SemaphoreType.DMA, pltpu.SemaphoreType.REGULAR
    anywhere = pl.BlockSpec(memory_space=pl.ANY)
    narrow, wide = [
        [(2, RG, FF), (2, RG, FF), (2, RD, D)],
        [(8, LAST)],
    ]
    outs = [S(s, BF) for s in narrow] + [S(s, F32) for s in wide]
    outs += [S((S2, D, FF), BF), S((S2, D, FF), BF), S((S2, FF, D), BF), S((S2, D, T), BF), S((S2, FF, T), BF), S((S2, NC, T, WIDE), F32), S((S2, T, COL), F32), S((T, D), BF)]
    outs += [S((Q, RG, WIDE), F32), S((Q, RG, WIDE), BF), S((Q, RG, WIDE), BF), S((T, FF), BF), S((T, FF), BF)]
    scratch = [V((T, D), BF), V((T, D), BF), V((RING, 2, RG, COL), BF), V((S3, 4 * RG, WIDE), BF), V((8, 8, LAST), F32)]
    scratch += [dma((len(UNITS), 8, 2)), dma((len(UNITS), 8, 2)), dma((len(UNITS), 2)), dma((RING, 2)), dma((Q, 4)), dma((RING, 6)), dma((3,)), dma((2,)), dma((2,)), dma((7,)), dma((7,))]
    scratch += [dma((3, 2)), dma((3, 8)), dma((4, 2)), regular, regular((2,))]
    return pl.pallas_call(
        kernel,
        out_shape=outs,
        in_specs=[anywhere] * 5,
        out_specs=[anywhere] * len(outs),
        scratch_shapes=scratch,
        compiler_params=pltpu.CompilerParams(collective_id=0, has_side_effects=YES, vmem_limit_bytes=67_000_000),
        name="step",
    )(x, dy, wg, wu, wd)[:4]


def adamw(w, m, v, g):
    m = 0.9 * m + 0.1 * g
    v = 0.95 * v + 0.05 * g * g
    step = m * lax.rsqrt(v + 1e-8) + 0.1 * w
    return (w - 0.02 * step).astype(BF), m, v


def solution(mesh):
    def step(x, dy, *arrays):
        weights, m, v = (arrays[i : i + 3] for i in (0, 3, 6))
        *gradients, squares = gradients_of(x[0], dy[0], *weights)
        count = mesh.shape["dp"] * sum(g.size for g in gradients)
        factor = jnp.minimum(1.0, 0.5 * lax.rsqrt(jnp.sum(squares) / count + 1e-30))
        new = [adamw(w.astype(F32), m, v, g.astype(F32) * factor) for w, m, v, g in zip(weights, m, v, gradients, strict=YES)]
        return tuple(one[which] for which in range(3) for one in new)

    states, cuts = P(("rep", "dp"), None, None), P(None, "dp", None)
    return jax.shard_map(
        step,
        mesh=mesh,
        in_specs=(states, states) + (cuts,) * 9,
        out_specs=(P("rep", "dp", None),) * 9,
        check_vma=NO,
    )
```

```python
import functools
import jax
import jax.numpy as jnp
from jax import lax
from jax.experimental import pallas as pl
from jax.experimental.pallas import tpu as pltpu
from jax.sharding import PartitionSpec as P

BF, F32 = jnp.bfloat16, jnp.float32
MESH = pl.DeviceIdType.MESH
T, D, FF = 2048, 1536, 4224
RG, RD = 192, 528
COL, WIDE, LAST = 256, 512, 128
TALL, HALF, MAIN = 1024, 768, 4096
NC = MAIN // COL
RDC, ND, PER = 176, 9, 26
Q, RING = 2 * PER, 13
DOWN, BOTH, TAIL = (RDC, WIDE), (RG, WIDE), (RG, COL)
OX, OY, OS, FX, FY, SX, SY, SD = range(8)
PARTS = ((0, 8), (8, 12), (12, NC), None)
NP = len(PARTS)
YES, NO = True, False
S2, S3, S4 = 2, 3, 4
PAIR = (0, 1)


def cut(i, n):
    return pl.ds(i * n, n) if isinstance(i, int) else pl.ds(pl.multiple_of(i * n, n), n)


def block(i, n):
    return pl.ds(i, n) if isinstance(i, int) else pl.ds(pl.multiple_of(i, 8), n)


def start(copies):
    for c in copies:
        c.start()


def wait(copies):
    for c in copies:
        c.wait()


def when(condition, do):
    if isinstance(condition, bool):
        if condition:
            do()
    else:
        pl.when(condition)(do)


def local(src, dst, sem):
    return pltpu.make_async_copy(src, dst, sem)


def dot(a, b, nt=NO):
    return lax.dot_general(a, b, (((1,), (int(nt),)), ((), ())), preferred_element_type=F32)


def gated(gate, up):
    s = jax.nn.sigmoid(gate)
    silu = gate * s
    return up * (s + silu * (1.0 - s)), silu, (silu * up).astype(BF)


def kernel(x, dy, wg, wu, wd, gg, gu, gd, squares, WGU, WD, aT, hT, R, Rt, h1, own, inx, iny, DGU,
           A, Y, dgi, d2r, sq, send, recv, keeps, dgi_sem, in_sem, out_sem, d2r_sem, d2s_sem, own_sem, sq_send, sq_recv, ld, ldl, st, credit, room):
    me = lax.axis_index("dp")
    core, y_, x_ = me % S2, (me // 2) % S2, me // 4
    at = lambda a, b, c: (a * 2 + b) * 2 + c
    xn, yn, dg, sib = at(1 - x_, y_, core), at(x_, 1 - y_, core), at(1 - x_, 1 - y_, core), at(x_, y_, 1 - core)
    other = lambda dev: dev + 1 - 2 * (dev % S2)
    everyone = [(me + k) % 8 for k in range(1, 8)]
    order = [other(dg), other(xn), other(yn), sib, dg, xn, yn, me]

    def remote(src, dst, sender, receiver, to):
        return pltpu.make_async_remote_copy(src, dst, sender, receiver, device_id={"dp": to}, device_id_type=MESH)

    def signal(sem, to):
        pl.semaphore_signal(sem, inc=1, device_id={"dp": to}, device_id_type=MESH)

    barrier = pltpu.get_barrier_semaphore()
    for dev in everyone:
        signal(barrier, dev)
    pl.semaphore_wait(barrier, len(everyone))

    to_whom = (xn, yn, sib, xn, yn, sib, sib, sib)
    whose = (me, me, me, yn, xn, xn, yn, dg)

    def half(u, p, dev):
        l, blocks = u[0], PARTS[u[1]]
        refs = (wg, wu, wd) if dev is None else (WGU.at[0], WGU.at[1], WD)
        ref, height, rows, top, cols = refs[2], RD, RD // 2, p * (RD // 2), pl.ds(0, D)
        if blocks:
            lo, hi = blocks[0] * COL, FF if blocks[1] == NC else blocks[1] * COL
            ref, height, rows, top, cols = refs[p], RG, RG, 0, pl.ds(lo, hi - lo)
        if dev is not None:
            top = pl.multiple_of(dev * height + top, 8)
        return ref.at[l, pl.ds(top, rows), cols]

    def hop(u, k, p):
        src = half(u, p, None if k <= OS else whose[k])
        i = u[0] * NP + u[1]
        return remote(src, half(u, p, whose[k]), send.at[i, k, p], recv.at[i, k, p], to_whom[k])

    def keep(u):
        return [local(half(u, p, None), half(u, p, me), keeps.at[u[0] * NP + u[1], p]) for p in PAIR]

    def first(u):
        start(hop(u, k, p) for k, p in ((OX, 0), (OY, 1), (OX, 1), (OY, 0), (OS, 0), (OS, 1)))

    def arrived(u, *which):
        for k, p in which:
            hop(u, k, p).wait_recv()

    def point1(u):
        arrived(u, (OX, 0), (OY, 1))
        start([hop(u, FY, 0), hop(u, FX, 1)])
        l, i = u
        if i + 1 < NP:
            first((l, i + 1))
        else:
            when(l < 1, lambda: first((l + 1, 0)))
        start([hop(u, SX, 0), hop(u, SY, 1)])

    def point2(u):
        arrived(u, (OX, 1), (OY, 0))
        start([hop(u, SX, 1), hop(u, SY, 0)])

    def point3(u):
        arrived(u, (FY, 0), (FX, 1))
        start(hop(u, SD, p) for p in PAIR)

    def point4(u):
        arrived(u, *((k, p) for k in (OS, SX, SY, SD) for p in PAIR))
        wait(keep(u))

    def rest(u):
        point2(u)
        point3(u)
        point4(u)

    def norm():
        @pl.loop(0, T // COL)
        def _(i):
            rows = cut(i, COL)
            wide = A[rows, :].astype(F32)
            scale = lax.rsqrt(jnp.mean(wide * wide, -1, keepdims=YES) + 1e-6)
            A[rows, :] = (wide * scale).astype(BF)

    def forward(H, hTs):
        def put_T(l, c, what):
            return local(hTs.at[c % S2], what.at[l, cut(c, COL), :], st.at[c % S2, 0])

        def transposed(l):
            n = D // COL

            @pl.loop(0, n)
            def _(c):
                pl.when(c >= 2)(lambda: put_T(l, c - 2, aT).wait())
                hTs[c % S2] = A[:, cut(c, COL)].T
                put_T(l, c, aT).start()

            wait(put_T(l, c, aT) for c in (n - 2, n - 1))

        def gate_up(l, Wb, r32):
            due = ((1, point1, 1), (3, point2, 1), (5, point3, 1), (8, point1, 2), (10, point2, 2), (11, point3, 2), (14, point1, 3))

            def get(j):
                return [local(WGU.at[i, l, :, cut(j, COL)], Wb.at[j % S3, :, cut(i, COL)], ld.at[j % S3, i]) for i in PAIR]

            def put(j):
                return [local(r32.at[j % S2], R.at[l, j], st.at[j % S2, 1]), put_T(l, j, hT)]

            def work(j, w, k, out):
                @pl.loop(0, 2)
                def _(i):
                    rows = cut(i, TALL)
                    r = dot(A[rows, :], Wb[k, :, pl.ds(0, 2 * w)])
                    by_gate, by_up, hid = gated(r[:, :w], r[:, w:])
                    r32[out, rows, pl.ds(0, w)] = by_gate
                    r32[out, rows, pl.ds(w, w)] = by_up
                    H[rows, pl.ds(MAIN, w) if w == LAST else cut(j, COL)] = hid
                    hTs[out, pl.ds(0, w), rows] = hid.T

            ws = [local(WGU.at[i, l, :, pl.ds(MAIN, LAST)], Wb.at[NC % S3, :, cut(i, LAST)], ld.at[NC % S3, i]) for i in PAIR]
            def begin(part):
                if part:
                    point4((l, part))
                lo = PARTS[part][0]
                start(get(lo) + get(lo + 1))

            begin(0)

            @pl.loop(0, NC)
            def _(j):
                for part in (1, 2):
                    pl.when(j == PARTS[part][0])(lambda: begin(part))
                wait(get(j))
                in_part = j + 2 < NC
                for _, lo in (PARTS[0], PARTS[1]):
                    in_part = jnp.logical_and(in_part, jnp.logical_and(j + 2 != lo, j + 1 != lo))
                pl.when(in_part)(lambda: start(get(j + 2)))
                pl.when(j == NC - 2)(lambda: start(ws))
                pl.when(j >= 2)(lambda: wait(put(j - 2)))
                work(j, COL, j % S3, j % S2)
                start(put(j))
                for i, point, part in due:
                    pl.when(j == i)(lambda: point((l, part)))

            wait(put(NC - 2) + ws)
            work(NC, LAST, NC % S3, 0)
            outs = [local(r32.at[0, :, pl.ds(0, COL)], Rt.at[l], st.at[0, 1]), local(hTs.at[0, pl.ds(0, LAST)], hT.at[l, pl.ds(MAIN, LAST), :], st.at[0, 0])]
            start(outs)
            wait(outs + put(NC - 1))

        def down(Wd, xs):
            n = D // COL

            def get(c):
                return [local(WD.at[0, :, cut(c, COL)], Wd.at[c % S2], ld.at[c % S2, 0]), local(x.at[:, cut(c, COL)], xs.at[c % S2], ld.at[c % S2, 1])]

            start(get(0))

            @pl.loop(0, n)
            def _(c):
                wait(get(c))
                pl.when(c + 1 < n)(lambda: start(get(c + 1)))

                @pl.loop(0, 2)
                def _(i):
                    rows = cut(i, TALL)
                    r = dot(H[rows, :], Wd[c % S2]).astype(BF)
                    A[rows, cut(c, COL)] = (xs[c % S2, rows, :].astype(F32) + r.astype(F32)).astype(BF)

                pl.when(c == 3)(lambda: point1((1, 0)))

        load = local(x, A, ld.at[0, 0])
        load.start()
        load.wait()

        @pl.loop(0, 2)
        def _(l):
            norm()
            transposed(l)
            pl.when(l == 0)(lambda: point1((0, 0)))
            rest((l, 0))
            pl.run_scoped(functools.partial(gate_up, l), pltpu.VMEM((S3, D, WIDE), BF), pltpu.VMEM((S2, T, WIDE), F32))

            @pl.when(l == 0)
            def _():
                rest((0, NP - 1))
                pl.run_scoped(down, pltpu.VMEM((S2, FF, COL), BF), pltpu.VMEM((S2, T, COL), BF))
                save = local(A, h1, ld.at[0, 0])
                save.start()
                save.wait()

    first((0, 0))
    by_y = local(dy, Y, st.at[3, 0])
    by_y.start()
    units = [(l, i) for l in PAIR for i in range(NP)]
    for u in units:
        start(keep(u))
    pl.run_scoped(forward, pltpu.VMEM((T, FF), BF), pltpu.VMEM((S2, COL, T), BF))

    def backward(sl, pend, d2s, ow):
        def d2d(q, kind):
            r, n = kind
            rows, cols = pl.ds(0, 4 * r), pl.ds(0, n)
            return remote(d2s.at[q % S2, rows, cols], d2r.at[q % S3, rows, cols], d2s_sem.at[q % S2], d2r_sem.at[q % S3], sib)

        def halves(kind):
            r, n = kind
            return pl.ds(0, r), pl.ds(0, n // 2), pl.ds(n // 2, n // 2)

        def outs(q, kind):
            s = q % RING
            rows, lo, hi = halves(kind)
            a, b, c = sl.at[s, 0], sl.at[s, 1], sl.at[s, 2]
            ends = [(a.at[rows, lo], dgi.at[s, 0, rows, lo], dgi_sem.at[s, 0], xn), (a.at[rows, hi], dgi.at[s, 1, rows, lo], dgi_sem.at[s, 1], yn)]
            ends += [(b.at[rows, lo], inx.at[q, rows, lo], in_sem.at[q, 0], xn), (c.at[rows, hi], iny.at[q, rows, hi], in_sem.at[q, 1], yn)]
            ends += [(b.at[rows, hi], inx.at[q, rows, hi], in_sem.at[q, 2], xn), (c.at[rows, lo], iny.at[q, rows, lo], in_sem.at[q, 3], yn)]
            return [remote(src, dst, out_sem.at[s, i], sem, to) for i, (src, dst, sem, to) in enumerate(ends)]

        def by_kind(q, do):
            c = q % PER
            pl.when(c < ND)(lambda: do(q, DOWN))
            pl.when(jnp.logical_and(c >= ND, c < PER - 1))(lambda: do(q, BOTH))
            pl.when(c == PER - 1)(lambda: do(q, TAIL))

        def release(q, kind):
            for c in outs(q, kind):
                c.wait_send()

        def put_own(q, kind):
            r, n = kind
            return local(ow.at[q % S2, pl.ds(0, r), pl.ds(0, n)], own.at[q, pl.ds(0, r), pl.ds(0, n)], own_sem.at[q % S2])

        def wait_own(q, kind):
            put_own(q, kind).wait()

        def before_add(q, kind):
            when(q >= RING, lambda: by_kind(jnp.int32(q - RING), release))
            c = d2d(q, kind)
            c.wait_recv()
            c.wait_send()
            when(q >= 2, lambda: by_kind(jnp.int32(q - 2), wait_own))

        def sums(q, kind, lhs, rhs):
            r, n = kind
            h, s = n // 2, q % RING
            rows, lo, hi = halves(kind)
            t = dot(lhs[pl.ds(4 * r, 4 * r), :], rhs) + d2r[q % S3, pl.ds(0, 4 * r), pl.ds(0, n)].astype(F32)
            sl[s, 0, rows, pl.ds(0, n)] = t[:r].astype(BF)
            sl[s, 1, rows, lo] = t[r : 2 * r, :h].astype(BF)
            pend[s, 1, rows, lo] = t[r : 2 * r, h:]
            sl[s, 2, rows, hi] = t[2 * r : 3 * r, h:].astype(BF)
            pend[s, 0, rows, lo] = t[2 * r : 3 * r, :h]
            ow[q % S2, rows, pl.ds(0, n)] = t[3 * r :]

        def theirs(q, kind, lhs, rhs):
            r, n = kind
            d2s[q % S2, pl.ds(0, 4 * r), pl.ds(0, n)] = dot(lhs[pl.ds(0, 4 * r), :], rhs).astype(BF)

        def after_add(q, kind):
            def room_there():
                for i in PAIR:
                    pl.semaphore_wait(room.at[i], 1)

            when(q >= RING, room_there)
            start(outs(q, kind)[:4])
            put_own(q, kind).start()
            when(q < Q - 3, lambda: signal(credit, sib))

        def send_d2d(q, kind):
            when(q >= 3, lambda: pl.semaphore_wait(credit, 1))
            d2d(q, kind).start()

        def serve(q, kind):
            s = q % RING
            rows, lo, hi = halves(kind)
            o = outs(q, kind)
            for c in o[:2]:
                c.wait_recv()
            sl[s, 2, rows, lo] = (pend[s, 0, rows, lo] + dgi[s, 0, rows, lo].astype(F32)).astype(BF)
            sl[s, 1, rows, hi] = (pend[s, 1, rows, lo] + dgi[s, 1, rows, lo].astype(F32)).astype(BF)
            start(o[4:])

            def done():
                for i, dev in enumerate((xn, yn)):
                    signal(room.at[i], dev)

            when(q < Q - RING, done)

        def serve_some(i, steps, lo, count, kind):
            a, b = (i * count) // steps, ((i + 1) * count) // steps
            pl.when(jnp.logical_and(b > a, jnp.logical_and(i >= 0, i < steps)))(lambda: serve(lo + a, kind))

        def down_gradient(base, l, then):
            def body(L):
                def get(t):
                    return [local(hT.at[l, block(dev * RD + t * RDC, RDC), :], L.at[t % S2, cut(b, RDC), :], ldl.at[t % S2, b]) for b, dev in enumerate(order)]

                def one(c, do_s, do_m):
                    q, e = base + c, c - 2
                    if do_s:
                        pl.when(c % S3 == 0)(lambda: wait(get(c // 3)))
                        pl.when(jnp.logical_and(c % S3 == 2, c < ND - 1))(lambda: start(get(c // 3 + 1)))
                    if do_m:
                        before_add(q - 2, DOWN)
                        sums(q - 2, DOWN, L.at[(e // 3) % S2], Y[:, cut(e % S3, WIDE)])
                    if do_s:
                        theirs(q, DOWN, L.at[(c // 3) % S2], Y[:, cut(c % S3, WIDE)])
                        send_d2d(q, DOWN)
                    if do_m:
                        after_add(q - 2, DOWN)

                start(get(0))
                @pl.loop(0, 2)
                def _(c):
                    one(c, YES, NO)

                @pl.loop(2, ND)
                def _(c):
                    one(c, YES, YES)
                    pl.when(jnp.logical_and(c == 2, l == 1))(lambda: point2((1, NP - 1)))
                    pl.when(jnp.logical_and(c == 7, l == 1))(lambda: point3((1, NP - 1)))

                then()

                @pl.loop(ND, ND + 2)
                def _(c):
                    one(c, NO, YES)

            pl.run_scoped(body, pltpu.VMEM((S2, 8 * RDC, T), BF))

        def layer_gradients(base, l):
            g = base + ND

            def outer(Rb):
                lhs = lambda L: [local(aT.at[l, block(dev * RG, RG), :], L.at[cut(b, RG), :], ldl.at[2, b]) for b, dev in enumerate(order)]
                is_last = lambda c: isinstance(c, int) and c == NC
                kind = lambda c: TAIL if is_last(c) else BOTH
                part = lambda dgu, c: dgu[c % S4, :, pl.ds(0, kind(c)[1])]

                def get(c):
                    k = c % S2
                    if is_last(c):
                        return [local(WD.at[l, pl.ds(MAIN, LAST), :], A.at[block(k * COL, LAST), :], ld.at[k, 0]), local(Rt.at[l], Rb.at[k, :, pl.ds(0, COL)], ld.at[k, 1])]
                    return [local(WD.at[l, cut(c, COL), :], A.at[cut(k, COL), :], ld.at[k, 0]), local(R.at[l, c], Rb.at[k], ld.at[k, 1])]

                def put(c, dgu):
                    w, cols = (LAST, pl.ds(MAIN, LAST)) if is_last(c) else (COL, cut(c, COL))
                    return [local(dgu.at[c % S4, :, cut(i, w)], DGU.at[i, :, cols], st.at[c % S4, i]) for i in PAIR]

                def step(s, L, dgu, do_f, do_s, do_m):
                    c, e = s - 1, s - 3
                    if do_f:
                        wait(get(s))
                        when(jnp.logical_and(s > 0, s < NC - 1) if not isinstance(s, int) else 0 < s < NC - 1, lambda: start(get(s + 1)))
                        when(s >= 4, lambda: wait(put(s - 4, dgu)))
                    if do_m:
                        before_add(g + e, kind(e))
                        sums(g + e, kind(e), L, part(dgu, e))
                    if do_s:
                        theirs(g + c, kind(c), L, part(dgu, c))
                    if do_f:
                        w = LAST if is_last(s) else COL
                        d = dot(Y[...], A[block(s % S2 * COL, w), :], nt=YES).astype(BF).astype(F32)
                        for i in PAIR:
                            dgu[s % S4, :, cut(i, w)] = (d * Rb[s % S2, :, cut(i, w)]).astype(BF)
                    if do_s:
                        send_d2d(g + c, kind(c))
                    if do_f:
                        start(put(s, dgu))
                    if do_m:
                        after_add(g + e, kind(e))

                def down_served(s):
                    serve_some(2 * s, 12, base, ND, DOWN)
                    serve_some(2 * s + 1, 12, base, ND, DOWN)

                def ahead():
                    pl.when(l == 1)(lambda: point4((1, NP - 1)))
                    start(get(0) + get(1))

                def body(L, dgu):
                    start(lhs(L))
                    step(0, L, dgu, YES, NO, NO)
                    down_served(jnp.int32(0))
                    wait(lhs(L))

                    @pl.loop(1, 3)
                    def _(s):
                        step(s, L, dgu, YES, YES, NO)
                        down_served(s)

                    @pl.loop(3, NC)
                    def _(s):
                        step(s, L, dgu, YES, YES, YES)
                        pl.when(s == NC - 2)(lambda: start(get(NC)))
                        down_served(s)
                        serve_some(s - 8, 8, g, 8, BOTH)

                    step(NC, L, dgu, YES, YES, YES)
                    serve(g + 8, BOTH)
                    step(NC + 1, L, dgu, NO, YES, YES)
                    step(NC + 2, L, dgu, NO, NO, YES)
                    step(NC + 3, L, dgu, NO, NO, YES)
                    for c in range(NC - 3, NC + 1):
                        wait(put(c, dgu))

                down_gradient(base, l, ahead)
                pl.run_scoped(body, pltpu.VMEM((D, T), BF), pltpu.VMEM((S4, T, WIDE), BF))

            pl.run_scoped(outer, pltpu.VMEM((S2, T, WIDE), F32))

        def input_gradient():
            m, n = T // WIDE, D // HALF
            steps = m * n

            def body(W, X, hb):
                def get_x(i):
                    src = DGU.at[i // steps]
                    return [local(src.at[cut(i % m * S4 + k, LAST), :], X.at[i % S2, cut(k, LAST), :], ldl.at[i % S2, k]) for k in range(S4)]

                def get_w(k):
                    return local(WGU.at[k // n, 1, cut(k % n, HALF), :], W.at[k % S2], ld.at[k % S2, 1])

                get_h = lambda i: local(h1.at[cut(i, LAST), :], hb.at[i % S4], st.at[i % S4, 0])
                start(get_h(i) for i in range(S4))
                get_w(0).start()
                start(get_x(0))

                @pl.loop(0, 2 * steps)
                def _(i):
                    k = i // m

                    @pl.when(i % m == 0)
                    def _():
                        get_w(k).wait()
                        pl.when(k < 2 * n - 1)(lambda: get_w(k + 1).start())

                    wait(get_x(i))
                    pl.when(i < 2 * steps - 1)(lambda: start(get_x(i + 1)))
                    r = dot(X[i % S2], W[k % S2], nt=YES).astype(BF)
                    place = (cut(i % m, WIDE), cut(k % n, HALF))
                    before = jnp.where(i < steps, 0.0, A[place].astype(F32))
                    A[place] = (before + r.astype(F32)).astype(BF)
                    serve_some(i, 13, ND + 9, 7, BOTH)

                serve(PER - 1, TAIL)

                @pl.loop(0, T // LAST)
                def _(i):
                    get_h(i).wait()
                    rows = cut(i, LAST)
                    f, b = hb[i % S4].astype(F32), A[rows, :].astype(F32)
                    ms = jnp.mean(f * f, -1, keepdims=YES) + 1e-6
                    scale = lax.rsqrt(ms)
                    c = jnp.sum(f * b, -1, keepdims=YES) * (-0.5 * (scale / ms)) * (1.0 / D)
                    back = (b * scale + c * (2.0 * f)).astype(BF)
                    Y[rows, :] = (Y[rows, :].astype(F32) + back.astype(F32)).astype(BF)
                    pl.when(i + S4 < T // LAST)(lambda: get_h(i + S4).start())

            V = pltpu.VMEM
            pl.run_scoped(body, V((S2, HALF, FF), BF), V((S2, WIDE, FF), BF), V((S4, LAST, D), BF))

        by_y.wait()

        @pl.loop(0, 2)
        def _(i):
            layer_gradients(i * PER, 1 - i)
            pl.when(i == 0)(input_gradient)

        for q in (Q - 2, Q - 1):
            by_kind(jnp.int32(q), wait_own)

        def finish(ob, ib, gb, acc):
            def get(q):
                return [local(own.at[q], ob.at[q % S3], ldl.at[q % S3, 0])] + [local(src.at[q], ib.at[q % S3, i], ldl.at[q % S3, i + 1]) for i, src in enumerate((inx, iny))]

            def fetch(q):
                def all_in(q, kind):
                    for c in outs(q, kind)[2:]:
                        c.wait_recv()

                by_kind(q, all_in)
                start(get(q))

            def put(q, kind):
                l, c, s = 1 - q // PER, q % PER, q % S2
                if kind == DOWN:
                    return [local(gb.at[s, pl.ds(0, RDC), :], gd.at[l, cut(c // 3, RDC), cut(c % S3, WIDE)], st.at[s, 0])]
                w = LAST if kind == TAIL else COL
                cols = pl.ds(MAIN, LAST) if kind == TAIL else cut(c - ND, COL)
                return [local(gb.at[s, :, cut(i, w)], dst.at[l, :, cols], st.at[s, i]) for i, dst in enumerate((gg, gu))]

            def one(q):
                pl.when(q < Q - 2)(lambda: fetch(q + 2))
                pl.when(q >= 2)(lambda: by_kind(q - 2, lambda q, kind: wait(put(q, kind))))
                wait(get(q))
                c, s = q % PER, q % S3
                height, width = jnp.where(c < ND, RDC, RG), jnp.where(c == PER - 1, COL, WIDE)
                inside = jnp.logical_and(lax.broadcasted_iota(jnp.int32, (RG, WIDE), 0) < height, lax.broadcasted_iota(jnp.int32, (RG, WIDE), 1) < width)
                g = (ob[s] + ib[s, 0].astype(F32) + ib[s, 1].astype(F32)).astype(BF)
                gb[q % S2] = g
                g = jnp.where(inside, g.astype(F32), 0.0)
                acc[...] += jnp.sum((g * g).reshape(RG // 8, 8, WIDE), 0)
                by_kind(q, lambda q, kind: start(put(q, kind)))

            acc[...] = jnp.zeros_like(acc)
            n = 6
            left = Q - 8
            fetch(jnp.int32(0))
            fetch(jnp.int32(1))

            @pl.loop(0, n * (Q - left))
            def _(q):
                pl.when(q % n == 0)(lambda: by_kind(left + q // n, serve))
                one(q)

            @pl.loop(n * (Q - left), Q)
            def _(q):
                one(q)

            for q in (Q - 2, Q - 1):
                by_kind(jnp.int32(q), lambda q, kind: wait(put(q, kind)))
            sq[me] = sum(acc[:, cut(i, LAST)] for i in range(WIDE // LAST))

        V = pltpu.VMEM
        pl.run_scoped(finish, V((S3, RG, WIDE), F32), V((S3, 2, RG, WIDE), BF), V((S2, RG, WIDE), BF), V((8, WIDE), F32))
        tell = [remote(sq.at[me], sq.at[me], sq_send.at[k], sq_recv.at[k], dev) for k, dev in enumerate(everyone)]
        start(tell)
        @pl.loop(Q - RING, Q)
        def _(q):
            by_kind(q, release)

        for u in units:
            for k in range(8):
                for p in ((1,) if k == FX else (0,) if k == FY else (0, 1)):
                    hop(u, k, p).wait_send()
        wait(tell)
        sq[0] = sum(sq[i] for i in range(8))
        out = local(sq.at[0], squares, ld.at[0, 0])
        out.start()
        out.wait()

    V = pltpu.VMEM
    pl.run_scoped(backward, V((RING, 3, RG, WIDE), BF), V((RING, 2, RG, COL), F32), V((S2, 4 * RG, WIDE), BF), V((S2, RG, WIDE), F32))


def gradients_of(x, dy, wg, wu, wd):
    S, V = jax.ShapeDtypeStruct, pltpu.VMEM
    dma, regular = pltpu.SemaphoreType.DMA, pltpu.SemaphoreType.REGULAR
    anywhere = pl.BlockSpec(memory_space=pl.ANY)
    narrow, wide = [
        [(2, RG, FF), (2, RG, FF), (2, RD, D)],
        [(8, LAST)],
    ]
    outs = [S(s, BF) for s in narrow] + [S(s, F32) for s in wide]
    outs += [S((2, 2, D, FF), BF), S((S2, FF, D), BF), S((S2, D, T), BF), S((S2, FF, T), BF), S((S2, NC, T, WIDE), F32), S((S2, T, COL), F32), S((T, D), BF)]
    outs += [S((Q, RG, WIDE), F32), S((Q, RG, WIDE), BF), S((Q, RG, WIDE), BF), S((2, T, FF), BF)]
    scratch = [V((T, D), BF), V((T, D), BF), V((RING, 2, RG, COL), BF), V((S3, 4 * RG, WIDE), BF), V((8, 8, LAST), F32)]
    scratch += [dma((2 * NP, 8, 2)), dma((2 * NP, 8, 2)), dma((2 * NP, 2)), dma((RING, 2)), dma((Q, 4)), dma((RING, 6)), dma((3,)), dma((2,)), dma((2,)), dma((7,)), dma((7,))]
    scratch += [dma((3, 2)), dma((3, 8)), dma((4, 2)), regular, regular((2,))]
    return pl.pallas_call(
        kernel,
        out_shape=outs,
        in_specs=[anywhere] * 5,
        out_specs=[anywhere] * len(outs),
        scratch_shapes=scratch,
        compiler_params=pltpu.CompilerParams(collective_id=0, has_side_effects=YES, vmem_limit_bytes=67_000_000),
        name="step",
    )(x, dy, wg, wu, wd)[:4]


STEPS = 4


def adamw_kernel(count, squares, *refs):
    factor = jnp.minimum(1.0, 0.5 * lax.rsqrt(jnp.sum(squares[...], keepdims=YES) / count + 1e-30))
    g, w, m, v, new_w, new_m, new_v = (refs[i : i + 3] for i in range(0, len(refs), 3))
    for i in range(3):
        by = g[i][...].astype(F32) * factor
        first = 0.9 * m[i][...] + 0.1 * by
        second = 0.95 * v[i][...] + 0.05 * by * by
        old = w[i][...].astype(F32)
        new_w[i][...] = (old - 0.02 * (first * lax.rsqrt(second + 1e-8) + 0.1 * old)).astype(BF)
        new_m[i][...] = first
        new_v[i][...] = second


def adamw(gradients, squares, count, weights, m, v):
    flat = [a.reshape(-1, a.shape[-1]) for a in (*gradients, *weights, *m, *v)]
    spec = lambda a: pl.BlockSpec((a.shape[0] // STEPS, a.shape[1]), lambda i: (i, 0))
    outs = [jax.ShapeDtypeStruct(a.shape, a.dtype) for a in flat[3:]]
    new = pl.pallas_call(
        functools.partial(adamw_kernel, count),
        grid=(STEPS,),
        out_shape=outs,
        in_specs=[pl.BlockSpec(squares.shape, lambda i: (0, 0))] + [spec(a) for a in flat],
        out_specs=[spec(a) for a in outs],
        compiler_params=pltpu.CompilerParams(vmem_limit_bytes=66_000_000),
        name="adamw",
    )(squares, *flat)
    return tuple(a.reshape(2, -1, a.shape[-1]) for a in new)


def solution(mesh):
    def step(x, dy, *arrays):
        weights, m, v = (arrays[i : i + 3] for i in (0, 3, 6))
        *gradients, squares = gradients_of(x[0], dy[0], *weights)
        return adamw(gradients, squares, mesh.shape["dp"] * sum(g.size for g in gradients), weights, m, v)

    states, cuts = P(("rep", "dp"), None, None), P(None, "dp", None)
    return jax.shard_map(
        step,
        mesh=mesh,
        in_specs=(states, states) + (cuts,) * 9,
        out_specs=(P("rep", "dp", None),) * 9,
        check_vma=NO,
    )
```

```python
import functools
import jax
import jax.numpy as jnp
from jax import lax
from jax.experimental import pallas as pl
from jax.experimental.pallas import tpu as pltpu
from jax.sharding import PartitionSpec as P

BF, F32 = jnp.bfloat16, jnp.float32
MESH = pl.DeviceIdType.MESH
T, D, FF = 2048, 1536, 4224
RG, RD = 192, 528
COL, WIDE, LAST = 256, 512, 128
TALL, HALF, MAIN = 1024, 768, 4096
NC = MAIN // COL
RDC, ND, PER = 176, 9, 26
Q, RING = 2 * PER, 13
DOWN, BOTH, TAIL = (RDC, WIDE), (RG, WIDE), (RG, COL)
OX, OY, OS, FX, FY, SX, SY, SD = range(8)
PARTS = ((0, 5), (5, 9), (9, 13), (13, NC), None)
NP = len(PARTS)
YES, NO = True, False
S2, S3, S4 = 2, 3, 4
PAIR = (0, 1)


def cut(i, n):
    return pl.ds(i * n, n) if isinstance(i, int) else pl.ds(pl.multiple_of(i * n, n), n)


def block(i, n):
    return pl.ds(i, n) if isinstance(i, int) else pl.ds(pl.multiple_of(i, 8), n)


def start(copies):
    for c in copies:
        c.start()


def wait(copies):
    for c in copies:
        c.wait()


def when(condition, do):
    if isinstance(condition, bool):
        if condition:
            do()
    else:
        pl.when(condition)(do)


def local(src, dst, sem):
    return pltpu.make_async_copy(src, dst, sem)


def dot(a, b, nt=NO):
    return lax.dot_general(a, b, (((1,), (int(nt),)), ((), ())), preferred_element_type=F32)


def gated(gate, up):
    s = jax.nn.sigmoid(gate)
    silu = gate * s
    return up * (s + silu * (1.0 - s)), silu, (silu * up).astype(BF)


def kernel(x, dy, wg, wu, wd, gg, gu, gd, squares, WGU, WD, aT, hT, R, Rt, h1, own, inx, iny, DGU,
           A, Y, dgi, d2r, sq, send, recv, keeps, dgi_sem, in_sem, out_sem, d2r_sem, d2s_sem, own_sem, sq_send, sq_recv, ld, ldl, st, credit, room):
    me = lax.axis_index("dp")
    core, y_, x_ = me % S2, (me // 2) % S2, me // 4
    at = lambda a, b, c: (a * 2 + b) * 2 + c
    xn, yn, dg, sib = at(1 - x_, y_, core), at(x_, 1 - y_, core), at(1 - x_, 1 - y_, core), at(x_, y_, 1 - core)
    other = lambda dev: dev + 1 - 2 * (dev % S2)
    everyone = [(me + k) % 8 for k in range(1, 8)]
    order = [other(dg), other(xn), other(yn), sib, dg, xn, yn, me]

    def remote(src, dst, sender, receiver, to):
        return pltpu.make_async_remote_copy(src, dst, sender, receiver, device_id={"dp": to}, device_id_type=MESH)

    def signal(sem, to):
        pl.semaphore_signal(sem, inc=1, device_id={"dp": to}, device_id_type=MESH)

    barrier = pltpu.get_barrier_semaphore()
    for dev in everyone:
        signal(barrier, dev)
    pl.semaphore_wait(barrier, len(everyone))

    to_whom = (xn, yn, sib, xn, yn, sib, sib, sib)
    whose = (me, me, me, yn, xn, xn, yn, dg)

    def half(u, p, dev):
        l, blocks = u[0], PARTS[u[1]]
        refs = (wg, wu, wd) if dev is None else (WGU.at[0], WGU.at[1], WD)
        ref, height, rows, top, cols = refs[2], RD, RD // 2, p * (RD // 2), pl.ds(0, D)
        if blocks:
            lo, hi = blocks[0] * COL, FF if blocks[1] == NC else blocks[1] * COL
            ref, height, rows, top, cols = refs[p], RG, RG, 0, pl.ds(lo, hi - lo)
        if dev is not None:
            top = pl.multiple_of(dev * height + top, 8)
        return ref.at[l, pl.ds(top, rows), cols]

    def hop(u, k, p):
        src = half(u, p, None if k <= OS else whose[k])
        i = u[0] * NP + u[1]
        return remote(src, half(u, p, whose[k]), send.at[i, k, p], recv.at[i, k, p], to_whom[k])

    def keep(u):
        return [local(half(u, p, None), half(u, p, me), keeps.at[u[0] * NP + u[1], p]) for p in PAIR]

    def first(u):
        start(hop(u, k, p) for k, p in ((OX, 0), (OY, 1), (OX, 1), (OY, 0), (OS, 0), (OS, 1)))

    def arrived(u, *which):
        for k, p in which:
            hop(u, k, p).wait_recv()

    def point1(u):
        arrived(u, (OX, 0), (OY, 1))
        start([hop(u, FY, 0), hop(u, FX, 1)])
        l, i = u
        if i + 1 < NP:
            first((l, i + 1))
        else:
            when(l < 1, lambda: first((l + 1, 0)))
        start([hop(u, SX, 0), hop(u, SY, 1)])

    def point2(u):
        arrived(u, (OX, 1), (OY, 0))
        start([hop(u, SX, 1), hop(u, SY, 0)])

    def point3(u):
        arrived(u, (FY, 0), (FX, 1))
        start(hop(u, SD, p) for p in PAIR)

    def point4(u):
        arrived(u, *((k, p) for k in (OS, SX, SY, SD) for p in PAIR))
        wait(keep(u))

    def rest(u):
        point2(u)
        point3(u)
        point4(u)

    def norm():
        @pl.loop(0, T // COL)
        def _(i):
            rows = cut(i, COL)
            wide = A[rows, :].astype(F32)
            scale = lax.rsqrt(jnp.mean(wide * wide, -1, keepdims=YES) + 1e-6)
            A[rows, :] = (wide * scale).astype(BF)

    def forward(H, hTs):
        def put_T(l, c, what):
            return local(hTs.at[c % S2], what.at[l, cut(c, COL), :], st.at[c % S2, 0])

        def transposed(l):
            n = D // COL

            @pl.loop(0, n)
            def _(c):
                pl.when(c >= 2)(lambda: put_T(l, c - 2, aT).wait())
                hTs[c % S2] = A[:, cut(c, COL)].T
                put_T(l, c, aT).start()

            wait(put_T(l, c, aT) for c in (n - 2, n - 1))

        def gate_up(l, Wb, r32):
            due = ((0, point2, 1), (2, point3, 1), (4, point1, 2), (6, point2, 2), (8, point3, 2), (9, point1, 3), (11, point2, 3), (12, point3, 3))
            due += ((NC - 1, point1, 4),)

            def get(j):
                return [local(WGU.at[i, l, :, cut(j, COL)], Wb.at[j % S3, :, cut(i, COL)], ld.at[j % S3, i]) for i in PAIR]

            def put(j):
                return [local(r32.at[j % S2], R.at[l, j], st.at[j % S2, 1]), put_T(l, j, hT)]

            def work(j, w, k, out):
                @pl.loop(0, 2)
                def _(i):
                    rows = cut(i, TALL)
                    r = dot(A[rows, :], Wb[k, :, pl.ds(0, 2 * w)])
                    by_gate, by_up, hid = gated(r[:, :w], r[:, w:])
                    r32[out, rows, pl.ds(0, w)] = by_gate
                    r32[out, rows, pl.ds(w, w)] = by_up
                    H[rows, pl.ds(MAIN, w) if w == LAST else cut(j, COL)] = hid
                    hTs[out, pl.ds(0, w), rows] = hid.T

            ws = [local(WGU.at[i, l, :, pl.ds(MAIN, LAST)], Wb.at[NC % S3, :, cut(i, LAST)], ld.at[NC % S3, i]) for i in PAIR]
            def begin(part):
                point4((l, part))
                lo = PARTS[part][0]
                start(get(lo) + get(lo + 1))

            begin(0)

            @pl.loop(0, NC)
            def _(j):
                for part in range(1, NP - 1):
                    pl.when(j == PARTS[part][0])(lambda: begin(part))
                wait(get(j))
                in_part = j + 2 < NC
                for lo, _ in PARTS[1 : NP - 1]:
                    in_part = jnp.logical_and(in_part, jnp.logical_and(j + 2 != lo, j + 1 != lo))
                pl.when(in_part)(lambda: start(get(j + 2)))
                pl.when(j == NC - 2)(lambda: start(ws))
                pl.when(j >= 2)(lambda: wait(put(j - 2)))
                work(j, COL, j % S3, j % S2)
                start(put(j))
                for i, point, part in due:
                    pl.when(j == i)(lambda: point((l, part)))

            wait(put(NC - 2) + ws)
            work(NC, LAST, NC % S3, 0)
            outs = [local(r32.at[0, :, pl.ds(0, COL)], Rt.at[l], st.at[0, 1]), local(hTs.at[0, pl.ds(0, LAST)], hT.at[l, pl.ds(MAIN, LAST), :], st.at[0, 0])]
            start(outs)
            wait(outs + put(NC - 1))

        def down(Wd, xs):
            n = D // COL

            def get(c):
                return [local(WD.at[0, :, cut(c, COL)], Wd.at[c % S2], ld.at[c % S2, 0]), local(x.at[:, cut(c, COL)], xs.at[c % S2], ld.at[c % S2, 1])]

            start(get(0))

            @pl.loop(0, n)
            def _(c):
                wait(get(c))
                pl.when(c + 1 < n)(lambda: start(get(c + 1)))

                @pl.loop(0, 2)
                def _(i):
                    rows = cut(i, TALL)
                    r = dot(H[rows, :], Wd[c % S2]).astype(BF)
                    A[rows, cut(c, COL)] = (xs[c % S2, rows, :].astype(F32) + r.astype(F32)).astype(BF)

                pl.when(c == 0)(lambda: point1((1, 0)))

        load = local(x, A, ld.at[0, 0])
        load.start()
        load.wait()

        @pl.loop(0, 2)
        def _(l):
            norm()
            transposed(l)

            @pl.when(l == 0)
            def _():
                point1((0, 0))
                point2((0, 0))
                point3((0, 0))

            point1((l, 1))
            pl.run_scoped(functools.partial(gate_up, l), pltpu.VMEM((S3, D, WIDE), BF), pltpu.VMEM((S2, T, WIDE), F32))

            @pl.when(l == 0)
            def _():
                rest((0, NP - 1))
                pl.run_scoped(down, pltpu.VMEM((S2, FF, COL), BF), pltpu.VMEM((S2, T, COL), BF))
                point2((1, 0))
                point3((1, 0))
                save = local(A, h1, ld.at[0, 0])
                save.start()
                save.wait()

    first((0, 0))
    by_y = local(dy, Y, st.at[3, 0])
    by_y.start()
    units = [(l, i) for l in PAIR for i in range(NP)]
    for u in units:
        start(keep(u))
    pl.run_scoped(forward, pltpu.VMEM((T, FF), BF), pltpu.VMEM((S2, COL, T), BF))

    def backward(sl, pend, d2s, ow):
        def d2d(q, kind):
            r, n = kind
            rows, cols = pl.ds(0, 4 * r), pl.ds(0, n)
            return remote(d2s.at[q % S2, rows, cols], d2r.at[q % S3, rows, cols], d2s_sem.at[q % S2], d2r_sem.at[q % S3], sib)

        def halves(kind):
            r, n = kind
            return pl.ds(0, r), pl.ds(0, n // 2), pl.ds(n // 2, n // 2)

        def outs(q, kind):
            s = q % RING
            rows, lo, hi = halves(kind)
            a, b, c = sl.at[s, 0], sl.at[s, 1], sl.at[s, 2]
            ends = [(a.at[rows, lo], dgi.at[s, 0, rows, lo], dgi_sem.at[s, 0], xn), (a.at[rows, hi], dgi.at[s, 1, rows, lo], dgi_sem.at[s, 1], yn)]
            ends += [(b.at[rows, lo], inx.at[q, rows, lo], in_sem.at[q, 0], xn), (c.at[rows, hi], iny.at[q, rows, hi], in_sem.at[q, 1], yn)]
            ends += [(b.at[rows, hi], inx.at[q, rows, hi], in_sem.at[q, 2], xn), (c.at[rows, lo], iny.at[q, rows, lo], in_sem.at[q, 3], yn)]
            return [remote(src, dst, out_sem.at[s, i], sem, to) for i, (src, dst, sem, to) in enumerate(ends)]

        def by_kind(q, do):
            c = q % PER
            pl.when(c < ND)(lambda: do(q, DOWN))
            pl.when(jnp.logical_and(c >= ND, c < PER - 1))(lambda: do(q, BOTH))
            pl.when(c == PER - 1)(lambda: do(q, TAIL))

        def release(q, kind):
            for c in outs(q, kind):
                c.wait_send()

        def put_own(q, kind):
            r, n = kind
            return local(ow.at[q % S2, pl.ds(0, r), pl.ds(0, n)], own.at[q, pl.ds(0, r), pl.ds(0, n)], own_sem.at[q % S2])

        def wait_own(q, kind):
            put_own(q, kind).wait()

        def before_add(q, kind):
            when(q >= RING, lambda: by_kind(jnp.int32(q - RING), release))
            c = d2d(q, kind)
            c.wait_recv()
            c.wait_send()
            when(q >= 2, lambda: by_kind(jnp.int32(q - 2), wait_own))

        def sums(q, kind, lhs, rhs):
            r, n = kind
            h, s = n // 2, q % RING
            rows, lo, hi = halves(kind)
            t = dot(lhs[pl.ds(4 * r, 4 * r), :], rhs) + d2r[q % S3, pl.ds(0, 4 * r), pl.ds(0, n)].astype(F32)
            sl[s, 0, rows, pl.ds(0, n)] = t[:r].astype(BF)
            sl[s, 1, rows, lo] = t[r : 2 * r, :h].astype(BF)
            pend[s, 1, rows, lo] = t[r : 2 * r, h:]
            sl[s, 2, rows, hi] = t[2 * r : 3 * r, h:].astype(BF)
            pend[s, 0, rows, lo] = t[2 * r : 3 * r, :h]
            ow[q % S2, rows, pl.ds(0, n)] = t[3 * r :]

        def theirs(q, kind, lhs, rhs):
            r, n = kind
            d2s[q % S2, pl.ds(0, 4 * r), pl.ds(0, n)] = dot(lhs[pl.ds(0, 4 * r), :], rhs).astype(BF)

        def after_add(q, kind):
            def room_there():
                for i in PAIR:
                    pl.semaphore_wait(room.at[i], 1)

            when(q >= RING, room_there)
            start(outs(q, kind)[:4])
            put_own(q, kind).start()
            when(q < Q - 3, lambda: signal(credit, sib))

        def send_d2d(q, kind):
            when(q >= 3, lambda: pl.semaphore_wait(credit, 1))
            d2d(q, kind).start()

        def serve(q, kind):
            s = q % RING
            rows, lo, hi = halves(kind)
            o = outs(q, kind)
            for c in o[:2]:
                c.wait_recv()
            sl[s, 2, rows, lo] = (pend[s, 0, rows, lo] + dgi[s, 0, rows, lo].astype(F32)).astype(BF)
            sl[s, 1, rows, hi] = (pend[s, 1, rows, lo] + dgi[s, 1, rows, lo].astype(F32)).astype(BF)
            start(o[4:])

            def done():
                for i, dev in enumerate((xn, yn)):
                    signal(room.at[i], dev)

            when(q < Q - RING, done)

        def serve_some(i, steps, lo, count, kind):
            a, b = (i * count) // steps, ((i + 1) * count) // steps
            pl.when(jnp.logical_and(b > a, jnp.logical_and(i >= 0, i < steps)))(lambda: serve(lo + a, kind))

        def down_gradient(base, l, then):
            def body(L):
                def get(t):
                    return [local(hT.at[l, block(dev * RD + t * RDC, RDC), :], L.at[t % S2, cut(b, RDC), :], ldl.at[t % S2, b]) for b, dev in enumerate(order)]

                def one(c, do_s, do_m):
                    q, e = base + c, c - 2
                    if do_s:
                        pl.when(c % S3 == 0)(lambda: wait(get(c // 3)))
                        pl.when(jnp.logical_and(c % S3 == 2, c < ND - 1))(lambda: start(get(c // 3 + 1)))
                    if do_m:
                        before_add(q - 2, DOWN)
                        sums(q - 2, DOWN, L.at[(e // 3) % S2], Y[:, cut(e % S3, WIDE)])
                    if do_s:
                        theirs(q, DOWN, L.at[(c // 3) % S2], Y[:, cut(c % S3, WIDE)])
                        send_d2d(q, DOWN)
                    if do_m:
                        after_add(q - 2, DOWN)

                start(get(0))
                @pl.loop(0, 2)
                def _(c):
                    one(c, YES, NO)

                @pl.loop(2, ND)
                def _(c):
                    one(c, YES, YES)
                    pl.when(jnp.logical_and(c == 4, l == 1))(lambda: point2((1, NP - 1)))

                pl.when(l == 1)(lambda: point3((1, NP - 1)))
                then()

                @pl.loop(ND, ND + 2)
                def _(c):
                    one(c, NO, YES)

            pl.run_scoped(body, pltpu.VMEM((S2, 8 * RDC, T), BF))

        def layer_gradients(base, l):
            g = base + ND

            def outer(Rb):
                lhs = lambda L: [local(aT.at[l, block(dev * RG, RG), :], L.at[cut(b, RG), :], ldl.at[2, b]) for b, dev in enumerate(order)]
                is_last = lambda c: isinstance(c, int) and c == NC
                kind = lambda c: TAIL if is_last(c) else BOTH
                part = lambda dgu, c: dgu[c % S4, :, pl.ds(0, kind(c)[1])]

                def get(c):
                    k = c % S2
                    if is_last(c):
                        return [local(WD.at[l, pl.ds(MAIN, LAST), :], A.at[block(k * COL, LAST), :], ld.at[k, 0]), local(Rt.at[l], Rb.at[k, :, pl.ds(0, COL)], ld.at[k, 1])]
                    return [local(WD.at[l, cut(c, COL), :], A.at[cut(k, COL), :], ld.at[k, 0]), local(R.at[l, c], Rb.at[k], ld.at[k, 1])]

                def put(c, dgu):
                    w, cols = (LAST, pl.ds(MAIN, LAST)) if is_last(c) else (COL, cut(c, COL))
                    return [local(dgu.at[c % S4, :, cut(i, w)], DGU.at[i, :, cols], st.at[c % S4, i]) for i in PAIR]

                def step(s, L, dgu, do_f, do_s, do_m):
                    c, e = s - 1, s - 3
                    if do_f:
                        if do_s:
                            wait(get(s))
                        when(jnp.logical_and(s > 0, s < NC - 1) if not isinstance(s, int) else 0 < s < NC - 1, lambda: start(get(s + 1)))
                        when(s >= 4, lambda: wait(put(s - 4, dgu)))
                    if do_m:
                        before_add(g + e, kind(e))
                        sums(g + e, kind(e), L, part(dgu, e))
                    if do_s:
                        theirs(g + c, kind(c), L, part(dgu, c))
                    if do_f:
                        w = LAST if is_last(s) else COL
                        d = dot(Y[...], A[block(s % S2 * COL, w), :], nt=YES).astype(BF).astype(F32)
                        for i in PAIR:
                            dgu[s % S4, :, cut(i, w)] = (d * Rb[s % S2, :, cut(i, w)]).astype(BF)
                    if do_s:
                        send_d2d(g + c, kind(c))
                    if do_f:
                        start(put(s, dgu))
                    if do_m:
                        after_add(g + e, kind(e))

                def down_served(s):
                    serve_some(2 * s, 12, base, ND, DOWN)
                    serve_some(2 * s + 1, 12, base, ND, DOWN)

                def ahead():
                    start(get(c)[1] for c in PAIR)

                def body(L, dgu):
                    pl.when(l == 1)(lambda: point4((1, NP - 1)))
                    get(0)[0].start()
                    wait(get(0))
                    start(lhs(L))
                    get(1)[0].start()
                    step(0, L, dgu, YES, NO, NO)
                    down_served(jnp.int32(0))
                    wait(lhs(L))

                    @pl.loop(1, 3)
                    def _(s):
                        step(s, L, dgu, YES, YES, NO)
                        down_served(s)

                    @pl.loop(3, NC)
                    def _(s):
                        step(s, L, dgu, YES, YES, YES)
                        pl.when(s == NC - 2)(lambda: start(get(NC)))
                        down_served(s)
                        serve_some(s - 8, 8, g, 8, BOTH)

                    step(NC, L, dgu, YES, YES, YES)
                    serve(g + 8, BOTH)
                    step(NC + 1, L, dgu, NO, YES, YES)
                    step(NC + 2, L, dgu, NO, NO, YES)
                    step(NC + 3, L, dgu, NO, NO, YES)
                    for c in range(NC - 3, NC + 1):
                        wait(put(c, dgu))

                down_gradient(base, l, ahead)
                pl.run_scoped(body, pltpu.VMEM((D, T), BF), pltpu.VMEM((S4, T, WIDE), BF))

            pl.run_scoped(outer, pltpu.VMEM((S2, T, WIDE), F32))

        def input_gradient():
            m, n = T // WIDE, D // HALF
            steps = m * n

            def body(W, X, hb):
                def get_x(i):
                    src = DGU.at[i // steps]
                    return [local(src.at[cut(i % m * S4 + k, LAST), :], X.at[i % S2, cut(k, LAST), :], ldl.at[i % S2, k]) for k in range(S4)]

                def get_w(k):
                    return local(WGU.at[k // n, 1, cut(k % n, HALF), :], W.at[k % S2], ld.at[k % S2, 1])

                get_h = lambda i: local(h1.at[cut(i, LAST), :], hb.at[i % S4], st.at[i % S4, 0])
                start(get_h(i) for i in range(S4))
                get_w(0).start()
                start(get_x(0))

                @pl.loop(0, 2 * steps)
                def _(i):
                    k = i // m

                    @pl.when(i % m == 0)
                    def _():
                        get_w(k).wait()
                        pl.when(k < 2 * n - 1)(lambda: get_w(k + 1).start())

                    wait(get_x(i))
                    pl.when(i < 2 * steps - 1)(lambda: start(get_x(i + 1)))
                    r = dot(X[i % S2], W[k % S2], nt=YES).astype(BF)
                    place = (cut(i % m, WIDE), cut(k % n, HALF))
                    before = jnp.where(i < steps, 0.0, A[place].astype(F32))
                    A[place] = (before + r.astype(F32)).astype(BF)
                    serve_some(i, 13, ND + 9, 7, BOTH)

                serve(PER - 1, TAIL)

                @pl.loop(0, T // LAST)
                def _(i):
                    get_h(i).wait()
                    rows = cut(i, LAST)
                    f, b = hb[i % S4].astype(F32), A[rows, :].astype(F32)
                    ms = jnp.mean(f * f, -1, keepdims=YES) + 1e-6
                    scale = lax.rsqrt(ms)
                    c = jnp.sum(f * b, -1, keepdims=YES) * (-0.5 * (scale / ms)) * (1.0 / D)
                    back = (b * scale + c * (2.0 * f)).astype(BF)
                    Y[rows, :] = (Y[rows, :].astype(F32) + back.astype(F32)).astype(BF)
                    pl.when(i + S4 < T // LAST)(lambda: get_h(i + S4).start())

            V = pltpu.VMEM
            pl.run_scoped(body, V((S2, HALF, FF), BF), V((S2, WIDE, FF), BF), V((S4, LAST, D), BF))

        by_y.wait()

        @pl.loop(0, 2)
        def _(i):
            layer_gradients(i * PER, 1 - i)
            pl.when(i == 0)(input_gradient)

        for q in (Q - 2, Q - 1):
            by_kind(jnp.int32(q), wait_own)

        def finish(ob, ib, gb, acc):
            def get(q):
                return [local(own.at[q], ob.at[q % S3], ldl.at[q % S3, 0])] + [local(src.at[q], ib.at[q % S3, i], ldl.at[q % S3, i + 1]) for i, src in enumerate((inx, iny))]

            def fetch(q):
                def all_in(q, kind):
                    for c in outs(q, kind)[2:]:
                        c.wait_recv()

                by_kind(q, all_in)
                start(get(q))

            def put(q, kind):
                l, c, s = 1 - q // PER, q % PER, q % S2
                if kind == DOWN:
                    return [local(gb.at[s, pl.ds(0, RDC), :], gd.at[l, cut(c // 3, RDC), cut(c % S3, WIDE)], st.at[s, 0])]
                w = LAST if kind == TAIL else COL
                cols = pl.ds(MAIN, LAST) if kind == TAIL else cut(c - ND, COL)
                return [local(gb.at[s, :, cut(i, w)], dst.at[l, :, cols], st.at[s, i]) for i, dst in enumerate((gg, gu))]

            def one(q):
                pl.when(q < Q - 2)(lambda: fetch(q + 2))
                pl.when(q >= 2)(lambda: by_kind(q - 2, lambda q, kind: wait(put(q, kind))))
                wait(get(q))
                c, s = q % PER, q % S3
                height, width = jnp.where(c < ND, RDC, RG), jnp.where(c == PER - 1, COL, WIDE)
                inside = jnp.logical_and(lax.broadcasted_iota(jnp.int32, (RG, WIDE), 0) < height, lax.broadcasted_iota(jnp.int32, (RG, WIDE), 1) < width)
                g = (ob[s] + ib[s, 0].astype(F32) + ib[s, 1].astype(F32)).astype(BF)
                gb[q % S2] = g
                g = jnp.where(inside, g.astype(F32), 0.0)
                acc[...] += jnp.sum((g * g).reshape(RG // 8, 8, WIDE), 0)
                by_kind(q, lambda q, kind: start(put(q, kind)))

            acc[...] = jnp.zeros_like(acc)
            n = 6
            left = Q - 8
            fetch(jnp.int32(0))
            fetch(jnp.int32(1))

            @pl.loop(0, n * (Q - left))
            def _(q):
                pl.when(q % n == 0)(lambda: by_kind(left + q // n, serve))
                one(q)

            @pl.loop(n * (Q - left), Q)
            def _(q):
                one(q)

            sq[...] = sum(acc[:, cut(i, LAST)] for i in range(WIDE // LAST))
            start(tell)
            for q in (Q - 2, Q - 1):
                by_kind(jnp.int32(q), lambda q, kind: wait(put(q, kind)))

        tell = [local(sq, squares.at[me], ld.at[0, 0])]
        tell += [remote(sq, squares.at[me], sq_send.at[k], sq_recv.at[k], dev) for k, dev in enumerate(everyone)]
        V = pltpu.VMEM
        pl.run_scoped(finish, V((S3, RG, WIDE), F32), V((S3, 2, RG, WIDE), BF), V((S2, RG, WIDE), BF), V((8, WIDE), F32))
        @pl.loop(Q - RING, Q)
        def _(q):
            by_kind(q, release)

        for u in units:
            for k in range(8):
                for p in ((1,) if k == FX else (0,) if k == FY else (0, 1)):
                    hop(u, k, p).wait_send()
        wait(tell)

    V = pltpu.VMEM
    pl.run_scoped(backward, V((RING, 3, RG, WIDE), BF), V((RING, 2, RG, COL), F32), V((S2, 4 * RG, WIDE), BF), V((S2, RG, WIDE), F32))


def gradients_of(x, dy, wg, wu, wd):
    S, V = jax.ShapeDtypeStruct, pltpu.VMEM
    dma, regular = pltpu.SemaphoreType.DMA, pltpu.SemaphoreType.REGULAR
    anywhere = pl.BlockSpec(memory_space=pl.ANY)
    narrow, wide = [
        [(2, RG, FF), (2, RG, FF), (2, RD, D)],
        [(8, 8, LAST)],
    ]
    outs = [S(s, BF) for s in narrow] + [S(s, F32) for s in wide]
    outs += [S((2, 2, D, FF), BF), S((S2, FF, D), BF), S((S2, D, T), BF), S((S2, FF, T), BF), S((S2, NC, T, WIDE), F32), S((S2, T, COL), F32), S((T, D), BF)]
    outs += [S((Q, RG, WIDE), F32), S((Q, RG, WIDE), BF), S((Q, RG, WIDE), BF), S((2, T, FF), BF)]
    scratch = [V((T, D), BF), V((T, D), BF), V((RING, 2, RG, COL), BF), V((S3, 4 * RG, WIDE), BF), V((8, LAST), F32)]
    scratch += [dma((2 * NP, 8, 2)), dma((2 * NP, 8, 2)), dma((2 * NP, 2)), dma((RING, 2)), dma((Q, 4)), dma((RING, 6)), dma((3,)), dma((2,)), dma((2,)), dma((7,)), dma((7,))]
    scratch += [dma((3, 2)), dma((3, 8)), dma((4, 2)), regular, regular((2,))]
    return pl.pallas_call(
        kernel,
        out_shape=outs,
        in_specs=[anywhere] * 5,
        out_specs=[anywhere] * len(outs),
        scratch_shapes=scratch,
        compiler_params=pltpu.CompilerParams(collective_id=0, has_side_effects=YES, vmem_limit_bytes=67_000_000),
        name="step",
    )(x, dy, wg, wu, wd)[:4]


STEPS = 4


def adamw_kernel(count, squares, *refs):
    factor = jnp.minimum(1.0, 0.5 * lax.rsqrt(jnp.sum(jnp.sum(squares[...], 0), keepdims=YES) / count + 1e-30))
    g, w, m, v, new_w, new_m, new_v = (refs[i : i + 3] for i in range(0, len(refs), 3))
    for i in range(3):
        by = g[i][...].astype(F32) * factor
        first = 0.9 * m[i][...] + 0.1 * by
        second = 0.95 * v[i][...] + 0.05 * by * by
        old = w[i][...].astype(F32)
        new_w[i][...] = (old - 0.02 * (first * lax.rsqrt(second + 1e-8) + 0.1 * old)).astype(BF)
        new_m[i][...] = first
        new_v[i][...] = second


def adamw(gradients, squares, count, weights, m, v):
    flat = [a.reshape(-1, a.shape[-1]) for a in (*gradients, *weights, *m, *v)]
    spec = lambda a: pl.BlockSpec((a.shape[0] // STEPS, a.shape[1]), lambda i: (i, 0))
    outs = [jax.ShapeDtypeStruct(a.shape, a.dtype) for a in flat[3:]]
    new = pl.pallas_call(
        functools.partial(adamw_kernel, count),
        grid=(STEPS,),
        out_shape=outs,
        in_specs=[pl.BlockSpec(squares.shape, lambda i: (0, 0, 0))] + [spec(a) for a in flat],
        out_specs=[spec(a) for a in outs],
        compiler_params=pltpu.CompilerParams(vmem_limit_bytes=66_000_000),
        name="adamw",
    )(squares, *flat)
    return tuple(a.reshape(2, -1, a.shape[-1]) for a in new)


def solution(mesh):
    def step(x, dy, *arrays):
        weights, m, v = (arrays[i : i + 3] for i in (0, 3, 6))
        *gradients, squares = gradients_of(x[0], dy[0], *weights)
        return adamw(gradients, squares, mesh.shape["dp"] * sum(g.size for g in gradients), weights, m, v)

    states, cuts = P(("rep", "dp"), None, None), P(None, "dp", None)
    return jax.shard_map(
        step,
        mesh=mesh,
        in_specs=(states, states) + (cuts,) * 9,
        out_specs=(P("rep", "dp", None),) * 9,
        check_vma=NO,
    )
```

```python
import functools
import jax
import jax.numpy as jnp
from jax import lax
from jax.experimental import pallas as pl
from jax.experimental.pallas import tpu as pltpu
from jax.sharding import PartitionSpec as P

BF, F32 = jnp.bfloat16, jnp.float32
MESH = pl.DeviceIdType.MESH
T, D, FF = 2048, 1536, 4224
RG, RD = 192, 528
COL, WIDE, LAST = 256, 512, 128
TALL, HALF, MAIN = 1024, 768, 4096
NC = MAIN // COL
RDC, ND, PER = 176, 9, 26
Q, RING = 2 * PER, 13
DOWN, BOTH, TAIL = (RDC, WIDE), (RG, WIDE), (RG, COL)
OX, OY, OS, FX, FY, SX, SY, SD = range(8)
PARTS = ((0, 5), (5, 9), (9, 13), (13, NC), None)
NP = len(PARTS)
YES, NO = True, False
S2, S3, S4 = 2, 3, 4
PAIR = (0, 1)


def cut(i, n):
    return pl.ds(i * n, n) if isinstance(i, int) else pl.ds(pl.multiple_of(i * n, n), n)


def block(i, n):
    return pl.ds(i, n) if isinstance(i, int) else pl.ds(pl.multiple_of(i, 8), n)


def start(copies):
    for c in copies:
        c.start()


def wait(copies):
    for c in copies:
        c.wait()


def when(condition, do):
    if isinstance(condition, bool):
        if condition:
            do()
    else:
        pl.when(condition)(do)


def local(src, dst, sem):
    return pltpu.make_async_copy(src, dst, sem)


def dot(a, b, nt=NO):
    return lax.dot_general(a, b, (((1,), (int(nt),)), ((), ())), preferred_element_type=F32)


def gated(gate, up):
    s = jax.nn.sigmoid(gate)
    silu = gate * s
    return up * (s + silu * (1.0 - s)), silu, (silu * up).astype(BF)


def kernel(x, dy, wg, wu, wd, gg, gu, gd, squares, WGU, WD, aT, hT, R, Rt, h1, own, inx, iny, DGU,
           A, Y, dgi, d2r, sq, send, recv, keeps, dgi_sem, in_sem, out_sem, d2r_sem, d2s_sem, own_sem, sq_send, sq_recv, ld, ldl, st, credit, room):
    me = lax.axis_index("dp")
    core, y_, x_ = me % S2, (me // 2) % S2, me // 4
    at = lambda a, b, c: (a * 2 + b) * 2 + c
    xn, yn, dg, sib = at(1 - x_, y_, core), at(x_, 1 - y_, core), at(1 - x_, 1 - y_, core), at(x_, y_, 1 - core)
    other = lambda dev: dev + 1 - 2 * (dev % S2)
    everyone = [(me + k) % 8 for k in range(1, 8)]
    order = [other(dg), other(xn), other(yn), sib, dg, xn, yn, me]

    def remote(src, dst, sender, receiver, to):
        return pltpu.make_async_remote_copy(src, dst, sender, receiver, device_id={"dp": to}, device_id_type=MESH)

    def signal(sem, to):
        pl.semaphore_signal(sem, inc=1, device_id={"dp": to}, device_id_type=MESH)

    barrier = pltpu.get_barrier_semaphore()
    for dev in everyone:
        signal(barrier, dev)
    pl.semaphore_wait(barrier, len(everyone))

    to_whom = (xn, yn, sib, xn, yn, sib, sib, sib)
    whose = (me, me, me, yn, xn, xn, yn, dg)

    def half(u, p, dev):
        l, blocks = u[0], PARTS[u[1]]
        refs = (wg, wu, wd) if dev is None else (WGU.at[0], WGU.at[1], WD)
        ref, height, rows, top, cols = refs[2], RD, RD // 2, p * (RD // 2), pl.ds(0, D)
        if blocks:
            lo, hi = blocks[0] * COL, FF if blocks[1] == NC else blocks[1] * COL
            ref, height, rows, top, cols = refs[p], RG, RG, 0, pl.ds(lo, hi - lo)
        if dev is not None:
            top = pl.multiple_of(dev * height + top, 8)
        return ref.at[l, pl.ds(top, rows), cols]

    def hop(u, k, p):
        src = half(u, p, None if k <= OS else whose[k])
        i = u[0] * NP + u[1]
        return remote(src, half(u, p, whose[k]), send.at[i, k, p], recv.at[i, k, p], to_whom[k])

    def keep(u):
        return [local(half(u, p, None), half(u, p, me), keeps.at[u[0] * NP + u[1], p]) for p in PAIR]

    def first(u):
        start(hop(u, k, p) for k, p in ((OX, 0), (OY, 1), (OX, 1), (OY, 0), (OS, 0), (OS, 1)))

    def arrived(u, *which):
        for k, p in which:
            hop(u, k, p).wait_recv()

    def point1(u):
        arrived(u, (OX, 0), (OY, 1))
        start([hop(u, FY, 0), hop(u, FX, 1)])
        l, i = u
        if i + 1 < NP:
            first((l, i + 1))
        else:
            when(l < 1, lambda: first((l + 1, 0)))
        start([hop(u, SX, 0), hop(u, SY, 1)])

    def point2(u):
        arrived(u, (OX, 1), (OY, 0))
        start([hop(u, SX, 1), hop(u, SY, 0)])

    def point3(u):
        arrived(u, (FY, 0), (FX, 1))
        start(hop(u, SD, p) for p in PAIR)

    def point4(u):
        arrived(u, *((k, p) for k in (OS, SX, SY, SD) for p in PAIR))
        wait(keep(u))

    def rest(u):
        point2(u)
        point3(u)
        point4(u)

    def norm():
        @pl.loop(0, T // COL)
        def _(i):
            rows = cut(i, COL)
            wide = A[rows, :].astype(F32)
            scale = lax.rsqrt(jnp.mean(wide * wide, -1, keepdims=YES) + 1e-6)
            A[rows, :] = (wide * scale).astype(BF)

    def forward(H, hTs):
        def put_T(l, c, what):
            return local(hTs.at[c % S2], what.at[l, cut(c, COL), :], st.at[c % S2, 0])

        def transposed(l):
            n = D // COL

            @pl.loop(0, n)
            def _(c):
                pl.when(c >= 2)(lambda: put_T(l, c - 2, aT).wait())
                hTs[c % S2] = A[:, cut(c, COL)].T
                put_T(l, c, aT).start()

            wait(put_T(l, c, aT) for c in (n - 2, n - 1))

        def gate_up(l, Wb, r32):
            due = ((0, point2, 1), (2, point3, 1), (4, point1, 2), (6, point2, 2), (8, point3, 2), (9, point1, 3), (11, point2, 3), (12, point3, 3))
            due += ((NC - 1, point1, 4),)

            def get(j):
                return [local(WGU.at[i, l, :, cut(j, COL)], Wb.at[j % S3, :, cut(i, COL)], ld.at[j % S3, i]) for i in PAIR]

            def put(j):
                return [local(r32.at[j % S2], R.at[l, j], st.at[j % S2, 1]), put_T(l, j, hT)]

            def work(j, w, k, out):
                @pl.loop(0, 2)
                def _(i):
                    rows = cut(i, TALL)
                    r = dot(A[rows, :], Wb[k, :, pl.ds(0, 2 * w)])
                    by_gate, by_up, hid = gated(r[:, :w], r[:, w:])
                    r32[out, rows, pl.ds(0, w)] = by_gate
                    r32[out, rows, pl.ds(w, w)] = by_up
                    H[rows, pl.ds(MAIN, w) if w == LAST else cut(j, COL)] = hid
                    hTs[out, pl.ds(0, w), rows] = hid.T

            ws = [local(WGU.at[i, l, :, pl.ds(MAIN, LAST)], Wb.at[NC % S3, :, cut(i, LAST)], ld.at[NC % S3, i]) for i in PAIR]
            def begin(part):
                point4((l, part))
                lo = PARTS[part][0]
                start(get(lo) + get(lo + 1))

            begin(0)

            @pl.loop(0, NC)
            def _(j):
                for part in range(1, NP - 1):
                    pl.when(j == PARTS[part][0])(lambda: begin(part))
                wait(get(j))
                in_part = j + 2 < NC
                for lo, _ in PARTS[1 : NP - 1]:
                    in_part = jnp.logical_and(in_part, jnp.logical_and(j + 2 != lo, j + 1 != lo))
                pl.when(in_part)(lambda: start(get(j + 2)))
                pl.when(j == NC - 2)(lambda: start(ws))
                pl.when(j >= 2)(lambda: wait(put(j - 2)))
                work(j, COL, j % S3, j % S2)
                start(put(j))
                for i, point, part in due:
                    pl.when(j == i)(lambda: point((l, part)))

            wait(put(NC - 2) + ws)
            work(NC, LAST, NC % S3, 0)
            outs = [local(r32.at[0, :, pl.ds(0, COL)], Rt.at[l], st.at[0, 1]), local(hTs.at[0, pl.ds(0, LAST)], hT.at[l, pl.ds(MAIN, LAST), :], st.at[0, 0])]
            start(outs)
            wait(outs + put(NC - 1))

        def down(Wd, xs):
            n = D // COL

            def get(c):
                return [local(WD.at[0, :, cut(c, COL)], Wd.at[c % S2], ld.at[c % S2, 0]), local(x.at[:, cut(c, COL)], xs.at[c % S2], ld.at[c % S2, 1])]

            start(get(0))

            @pl.loop(0, n)
            def _(c):
                wait(get(c))
                pl.when(c + 1 < n)(lambda: start(get(c + 1)))

                @pl.loop(0, 2)
                def _(i):
                    rows = cut(i, TALL)
                    r = dot(H[rows, :], Wd[c % S2]).astype(BF)
                    A[rows, cut(c, COL)] = (xs[c % S2, rows, :].astype(F32) + r.astype(F32)).astype(BF)

                pl.when(c == 0)(lambda: point1((1, 0)))

        load = local(x, A, ld.at[0, 0])
        load.start()
        load.wait()

        @pl.loop(0, 2)
        def _(l):
            norm()
            transposed(l)

            @pl.when(l == 0)
            def _():
                point1((0, 0))
                point2((0, 0))
                point3((0, 0))

            point1((l, 1))
            pl.run_scoped(functools.partial(gate_up, l), pltpu.VMEM((S3, D, WIDE), BF), pltpu.VMEM((S2, T, WIDE), F32))

            @pl.when(l == 0)
            def _():
                rest((0, NP - 1))
                pl.run_scoped(down, pltpu.VMEM((S2, FF, COL), BF), pltpu.VMEM((S2, T, COL), BF))
                point2((1, 0))
                point3((1, 0))
                save = local(A, h1, ld.at[0, 0])
                save.start()
                save.wait()

    first((0, 0))
    by_y = local(dy, Y, st.at[3, 0])
    by_y.start()
    units = [(l, i) for l in PAIR for i in range(NP)]
    for u in units:
        start(keep(u))
    pl.run_scoped(forward, pltpu.VMEM((T, FF), BF), pltpu.VMEM((S2, COL, T), BF))

    def backward(sl, pend, d2s, ow):
        def d2d(q, kind):
            r, n = kind
            rows, cols = pl.ds(0, 4 * r), pl.ds(0, n)
            return remote(d2s.at[q % S2, rows, cols], d2r.at[q % S3, rows, cols], d2s_sem.at[q % S2], d2r_sem.at[q % S3], sib)

        def halves(kind):
            r, n = kind
            return pl.ds(0, r), pl.ds(0, n // 2), pl.ds(n // 2, n // 2)

        def outs(q, kind):
            s = q % RING
            rows, lo, hi = halves(kind)
            a, b, c = sl.at[s, 0], sl.at[s, 1], sl.at[s, 2]
            ends = [(a.at[rows, lo], dgi.at[s, 0, rows, lo], dgi_sem.at[s, 0], xn), (a.at[rows, hi], dgi.at[s, 1, rows, lo], dgi_sem.at[s, 1], yn)]
            ends += [(b.at[rows, lo], inx.at[q, rows, lo], in_sem.at[q, 0], xn), (c.at[rows, hi], iny.at[q, rows, hi], in_sem.at[q, 1], yn)]
            ends += [(b.at[rows, hi], inx.at[q, rows, hi], in_sem.at[q, 2], xn), (c.at[rows, lo], iny.at[q, rows, lo], in_sem.at[q, 3], yn)]
            return [remote(src, dst, out_sem.at[s, i], sem, to) for i, (src, dst, sem, to) in enumerate(ends)]

        def by_kind(q, do):
            c = q % PER
            pl.when(c < ND)(lambda: do(q, DOWN))
            pl.when(jnp.logical_and(c >= ND, c < PER - 1))(lambda: do(q, BOTH))
            pl.when(c == PER - 1)(lambda: do(q, TAIL))

        def release(q, kind):
            for c in outs(q, kind):
                c.wait_send()

        def put_own(q, kind):
            r, n = kind
            return local(ow.at[q % S2, pl.ds(0, r), pl.ds(0, n)], own.at[q, pl.ds(0, r), pl.ds(0, n)], own_sem.at[q % S2])

        def wait_own(q, kind):
            put_own(q, kind).wait()

        def before_add(q, kind):
            when(q >= RING, lambda: by_kind(jnp.int32(q - RING), release))
            c = d2d(q, kind)
            c.wait_recv()
            c.wait_send()
            when(q >= 2, lambda: by_kind(jnp.int32(q - 2), wait_own))

        def sums(q, kind, lhs, rhs):
            r, n = kind
            h, s = n // 2, q % RING
            rows, lo, hi = halves(kind)
            t = dot(lhs[pl.ds(4 * r, 4 * r), :], rhs) + d2r[q % S3, pl.ds(0, 4 * r), pl.ds(0, n)].astype(F32)
            sl[s, 0, rows, pl.ds(0, n)] = t[:r].astype(BF)
            sl[s, 1, rows, lo] = t[r : 2 * r, :h].astype(BF)
            pend[s, 1, rows, lo] = t[r : 2 * r, h:]
            sl[s, 2, rows, hi] = t[2 * r : 3 * r, h:].astype(BF)
            pend[s, 0, rows, lo] = t[2 * r : 3 * r, :h]
            ow[q % S2, rows, pl.ds(0, n)] = t[3 * r :]

        def theirs(q, kind, lhs, rhs):
            r, n = kind
            d2s[q % S2, pl.ds(0, 4 * r), pl.ds(0, n)] = dot(lhs[pl.ds(0, 4 * r), :], rhs).astype(BF)

        def after_add(q, kind):
            def room_there():
                for i in PAIR:
                    pl.semaphore_wait(room.at[i], 1)

            when(q >= RING, room_there)
            start(outs(q, kind)[:4])
            put_own(q, kind).start()
            when(q < Q - 3, lambda: signal(credit, sib))

        def send_d2d(q, kind):
            when(q >= 3, lambda: pl.semaphore_wait(credit, 1))
            d2d(q, kind).start()

        def serve(q, kind):
            s = q % RING
            rows, lo, hi = halves(kind)
            o = outs(q, kind)
            for c in o[:2]:
                c.wait_recv()
            sl[s, 2, rows, lo] = (pend[s, 0, rows, lo] + dgi[s, 0, rows, lo].astype(F32)).astype(BF)
            sl[s, 1, rows, hi] = (pend[s, 1, rows, lo] + dgi[s, 1, rows, lo].astype(F32)).astype(BF)
            start(o[4:])

            def done():
                for i, dev in enumerate((xn, yn)):
                    signal(room.at[i], dev)

            when(q < Q - RING, done)

        def serve_some(i, steps, lo, count, kind):
            a, b = (i * count) // steps, ((i + 1) * count) // steps
            pl.when(jnp.logical_and(b > a, jnp.logical_and(i >= 0, i < steps)))(lambda: serve(lo + a, kind))

        def down_gradient(base, l, then):
            def body(L, hb):
                def get(t):
                    return [local(hT.at[l, block(dev * RD + t * RDC, RDC), :], L.at[t % S2, cut(b, RDC), :], ldl.at[t % S2, b]) for b, dev in enumerate(order)]

                def one(c, do_s, do_m):
                    q, e = base + c, c - 2
                    if do_s:
                        pl.when(c % S3 == 0)(lambda: wait(get(c // 3)))
                        pl.when(jnp.logical_and(c % S3 == 2, c < ND - 1))(lambda: start(get(c // 3 + 1)))
                    if do_m:
                        before_add(q - 2, DOWN)
                        sums(q - 2, DOWN, L.at[(e // 3) % S2], Y[:, cut(e % S3, WIDE)])
                    if do_s:
                        theirs(q, DOWN, L.at[(c // 3) % S2], Y[:, cut(c % S3, WIDE)])
                        send_d2d(q, DOWN)
                    if do_m:
                        after_add(q - 2, DOWN)

                get_h = lambda i: local(h1.at[cut(i, LAST), :], hb.at[i % S4], st.at[i % S4, 0])

                def back_through_norm():
                    start(get_h(i) for i in range(S4))

                    @pl.loop(0, T // LAST)
                    def _(i):
                        get_h(i).wait()
                        rows = cut(i, LAST)
                        f, b = hb[i % S4].astype(F32), A[rows, :].astype(F32)
                        ms = jnp.mean(f * f, -1, keepdims=YES) + 1e-6
                        scale = lax.rsqrt(ms)
                        c = jnp.sum(f * b, -1, keepdims=YES) * (scale / ms) * (-1.0 / D)
                        back = (b * scale + c * f).astype(BF)
                        Y[rows, :] = (Y[rows, :].astype(F32) + back.astype(F32)).astype(BF)
                        pl.when(i + S4 < T // LAST)(lambda: get_h(i + S4).start())

                start(get(0))
                pl.when(l == 0)(back_through_norm)

                @pl.loop(0, 2)
                def _(c):
                    one(c, YES, NO)

                @pl.loop(2, ND)
                def _(c):
                    one(c, YES, YES)
                    pl.when(jnp.logical_and(c == 4, l == 1))(lambda: point2((1, NP - 1)))

                pl.when(l == 1)(lambda: point3((1, NP - 1)))
                then()

                @pl.loop(ND, ND + 2)
                def _(c):
                    one(c, NO, YES)

            pl.run_scoped(body, pltpu.VMEM((S2, 8 * RDC, T), BF), pltpu.VMEM((S4, LAST, D), BF))

        def layer_gradients(base, l):
            g = base + ND

            def outer(Rb):
                lhs = lambda L: [local(aT.at[l, block(dev * RG, RG), :], L.at[cut(b, RG), :], ldl.at[2, b]) for b, dev in enumerate(order)]
                is_last = lambda c: isinstance(c, int) and c == NC
                kind = lambda c: TAIL if is_last(c) else BOTH
                part = lambda dgu, c: dgu[c % S4, :, pl.ds(0, kind(c)[1])]

                def get(c):
                    k = c % S2
                    if is_last(c):
                        return [local(WD.at[l, pl.ds(MAIN, LAST), :], A.at[block(k * COL, LAST), :], ld.at[k, 0]), local(Rt.at[l], Rb.at[k, :, pl.ds(0, COL)], ld.at[k, 1])]
                    return [local(WD.at[l, cut(c, COL), :], A.at[cut(k, COL), :], ld.at[k, 0]), local(R.at[l, c], Rb.at[k], ld.at[k, 1])]

                def put(c, dgu):
                    w, cols = (LAST, pl.ds(MAIN, LAST)) if is_last(c) else (COL, cut(c, COL))
                    return [local(dgu.at[c % S4, :, cut(i, w)], DGU.at[i, :, cols], st.at[c % S4, i]) for i in PAIR]

                def step(s, L, dgu, do_f, do_s, do_m):
                    c, e = s - 1, s - 3
                    if do_f:
                        if do_s:
                            wait(get(s))
                        when(jnp.logical_and(s > 0, s < NC - 1) if not isinstance(s, int) else 0 < s < NC - 1, lambda: start(get(s + 1)))
                        when(s >= 4, lambda: wait(put(s - 4, dgu)))
                    if do_m:
                        before_add(g + e, kind(e))
                        sums(g + e, kind(e), L, part(dgu, e))
                    if do_s:
                        theirs(g + c, kind(c), L, part(dgu, c))
                    if do_f:
                        w = LAST if is_last(s) else COL
                        d = dot(Y[...], A[block(s % S2 * COL, w), :], nt=YES).astype(BF).astype(F32)
                        for i in PAIR:
                            dgu[s % S4, :, cut(i, w)] = (d * Rb[s % S2, :, cut(i, w)]).astype(BF)
                    if do_s:
                        send_d2d(g + c, kind(c))
                    if do_f:
                        start(put(s, dgu))
                    if do_m:
                        after_add(g + e, kind(e))

                def down_served(s):
                    serve_some(2 * s, 12, base, ND, DOWN)
                    serve_some(2 * s + 1, 12, base, ND, DOWN)

                def ahead():
                    start(get(c)[1] for c in PAIR)

                def body(L, dgu):
                    pl.when(l == 1)(lambda: point4((1, NP - 1)))
                    start(get(c)[0] for c in PAIR)
                    wait(get(0))
                    start(lhs(L))
                    step(0, L, dgu, YES, NO, NO)
                    down_served(jnp.int32(0))
                    wait(lhs(L))

                    @pl.loop(1, 3)
                    def _(s):
                        step(s, L, dgu, YES, YES, NO)
                        down_served(s)

                    @pl.loop(3, NC)
                    def _(s):
                        step(s, L, dgu, YES, YES, YES)
                        pl.when(s == NC - 2)(lambda: start(get(NC)))
                        down_served(s)
                        serve_some(s - 8 - l, 8, g, 8, BOTH)

                    step(NC, L, dgu, YES, YES, YES)
                    serve(g + 8 - l, BOTH)
                    step(NC + 1, L, dgu, NO, YES, YES)
                    step(NC + 2, L, dgu, NO, NO, YES)
                    step(NC + 3, L, dgu, NO, NO, YES)
                    for c in range(NC - 3, NC + 1):
                        wait(put(c, dgu))

                down_gradient(base, l, ahead)
                pl.run_scoped(body, pltpu.VMEM((D, T), BF), pltpu.VMEM((S4, T, WIDE), BF))

            pl.run_scoped(outer, pltpu.VMEM((S2, T, WIDE), F32))

        def input_gradient():
            m, n = T // WIDE, D // HALF
            steps = m * n

            def body(W, X):
                def get_x(i):
                    src = DGU.at[i // steps]
                    return [local(src.at[cut(i % m * S4 + k, LAST), :], X.at[i % S2, cut(k, LAST), :], ldl.at[i % S2, k]) for k in range(S4)]

                def get_w(k):
                    return local(WGU.at[k // n, 1, cut(k % n, HALF), :], W.at[k % S2], ld.at[k % S2, 1])

                get_w(0).start()
                start(get_x(0))

                @pl.loop(0, 2 * steps)
                def _(i):
                    k = i // m

                    @pl.when(i % m == 0)
                    def _():
                        get_w(k).wait()
                        pl.when(k < 2 * n - 1)(lambda: get_w(k + 1).start())

                    wait(get_x(i))
                    pl.when(i < 2 * steps - 1)(lambda: start(get_x(i + 1)))
                    r = dot(X[i % S2], W[k % S2], nt=YES).astype(BF)
                    place = (cut(i % m, WIDE), cut(k % n, HALF))
                    before = jnp.where(i < steps, 0.0, A[place].astype(F32))
                    A[place] = (before + r.astype(F32)).astype(BF)
                    serve_some(i, 14, ND + 8, 8, BOTH)

                serve(PER - 1, TAIL)

            pl.run_scoped(body, pltpu.VMEM((S2, HALF, FF), BF), pltpu.VMEM((S2, WIDE, FF), BF))

        by_y.wait()

        @pl.loop(0, 2)
        def _(i):
            layer_gradients(i * PER, 1 - i)
            pl.when(i == 0)(input_gradient)

        for q in (Q - 2, Q - 1):
            by_kind(jnp.int32(q), wait_own)

        def finish(ob, ib, gb, acc):
            def get(q):
                return [local(own.at[q], ob.at[q % S3], ldl.at[q % S3, 0])] + [local(src.at[q], ib.at[q % S3, i], ldl.at[q % S3, i + 1]) for i, src in enumerate((inx, iny))]

            def fetch(q):
                def all_in(q, kind):
                    for c in outs(q, kind)[2:]:
                        c.wait_recv()

                by_kind(q, all_in)
                start(get(q))

            def put(q, kind):
                l, c, s = 1 - q // PER, q % PER, q % S2
                if kind == DOWN:
                    return [local(gb.at[s, pl.ds(0, RDC), :], gd.at[l, cut(c // 3, RDC), cut(c % S3, WIDE)], st.at[s, 0])]
                w = LAST if kind == TAIL else COL
                cols = pl.ds(MAIN, LAST) if kind == TAIL else cut(c - ND, COL)
                return [local(gb.at[s, :, cut(i, w)], dst.at[l, :, cols], st.at[s, i]) for i, dst in enumerate((gg, gu))]

            def one(q):
                pl.when(q < Q - 2)(lambda: fetch(q + 2))
                pl.when(q >= 2)(lambda: by_kind(q - 2, lambda q, kind: wait(put(q, kind))))
                wait(get(q))
                c, s = q % PER, q % S3
                height, width = jnp.where(c < ND, RDC, RG), jnp.where(c == PER - 1, COL, WIDE)
                inside = jnp.logical_and(lax.broadcasted_iota(jnp.int32, (RG, WIDE), 0) < height, lax.broadcasted_iota(jnp.int32, (RG, WIDE), 1) < width)
                g = (ob[s] + ib[s, 0].astype(F32) + ib[s, 1].astype(F32)).astype(BF)
                gb[q % S2] = g
                g = jnp.where(inside, g.astype(F32), 0.0)
                acc[...] += jnp.sum((g * g).reshape(RG // 8, 8, WIDE), 0)
                by_kind(q, lambda q, kind: start(put(q, kind)))

            acc[...] = jnp.zeros_like(acc)
            n = 6
            left = Q - 8
            fetch(jnp.int32(0))
            fetch(jnp.int32(1))

            @pl.loop(0, n * (Q - left))
            def _(q):
                pl.when(q % n == 0)(lambda: by_kind(left + q // n, serve))
                one(q)

            @pl.loop(n * (Q - left), Q)
            def _(q):
                one(q)

            sq[...] = sum(acc[:, cut(i, LAST)] for i in range(WIDE // LAST))
            start(tell)
            for q in (Q - 2, Q - 1):
                by_kind(jnp.int32(q), lambda q, kind: wait(put(q, kind)))

        tell = [local(sq, squares.at[me], ld.at[0, 0])]
        tell += [remote(sq, squares.at[me], sq_send.at[k], sq_recv.at[k], dev) for k, dev in enumerate(everyone)]
        V = pltpu.VMEM
        pl.run_scoped(finish, V((S3, RG, WIDE), F32), V((S3, 2, RG, WIDE), BF), V((S2, RG, WIDE), BF), V((8, WIDE), F32))
        @pl.loop(Q - RING, Q)
        def _(q):
            by_kind(q, release)

        for u in units:
            for k in range(8):
                for p in ((1,) if k == FX else (0,) if k == FY else (0, 1)):
                    hop(u, k, p).wait_send()
        wait(tell)

    V = pltpu.VMEM
    pl.run_scoped(backward, V((RING, 3, RG, WIDE), BF), V((RING, 2, RG, COL), F32), V((S2, 4 * RG, WIDE), BF), V((S2, RG, WIDE), F32))


def gradients_of(x, dy, wg, wu, wd):
    S, V = jax.ShapeDtypeStruct, pltpu.VMEM
    dma, regular = pltpu.SemaphoreType.DMA, pltpu.SemaphoreType.REGULAR
    anywhere = pl.BlockSpec(memory_space=pl.ANY)
    narrow, wide = [
        [(2, RG, FF), (2, RG, FF), (2, RD, D)],
        [(8, 8, LAST)],
    ]
    outs = [S(s, BF) for s in narrow] + [S(s, F32) for s in wide]
    outs += [S((2, 2, D, FF), BF), S((S2, FF, D), BF), S((S2, D, T), BF), S((S2, FF, T), BF), S((S2, NC, T, WIDE), F32), S((S2, T, COL), F32), S((T, D), BF)]
    outs += [S((Q, RG, WIDE), F32), S((Q, RG, WIDE), BF), S((Q, RG, WIDE), BF), S((2, T, FF), BF)]
    scratch = [V((T, D), BF), V((T, D), BF), V((RING, 2, RG, COL), BF), V((S3, 4 * RG, WIDE), BF), V((8, LAST), F32)]
    scratch += [dma((2 * NP, 8, 2)), dma((2 * NP, 8, 2)), dma((2 * NP, 2)), dma((RING, 2)), dma((Q, 4)), dma((RING, 6)), dma((3,)), dma((2,)), dma((2,)), dma((7,)), dma((7,))]
    scratch += [dma((3, 2)), dma((3, 8)), dma((4, 2)), regular, regular((2,))]
    return pl.pallas_call(
        kernel,
        out_shape=outs,
        in_specs=[anywhere] * 5,
        out_specs=[anywhere] * len(outs),
        scratch_shapes=scratch,
        compiler_params=pltpu.CompilerParams(collective_id=0, has_side_effects=YES, vmem_limit_bytes=67_000_000),
        name="step",
    )(x, dy, wg, wu, wd)[:4]


STEPS = 4


def adamw_kernel(count, squares, *refs):
    factor = jnp.minimum(1.0, 0.5 * lax.rsqrt(jnp.sum(jnp.sum(squares[...], 0), keepdims=YES) / count + 1e-30))
    g, w, m, v, new_w, new_m, new_v = (refs[i : i + 3] for i in range(0, len(refs), 3))
    for i in range(3):
        by = g[i][...].astype(F32) * factor
        first = 0.9 * m[i][...] + 0.1 * by
        second = 0.95 * v[i][...] + 0.05 * by * by
        old = w[i][...].astype(F32)
        new_w[i][...] = (old - 0.02 * (first * lax.rsqrt(second + 1e-8) + 0.1 * old)).astype(BF)
        new_m[i][...] = first
        new_v[i][...] = second


def adamw(gradients, squares, count, weights, m, v):
    flat = [a.reshape(-1, a.shape[-1]) for a in (*gradients, *weights, *m, *v)]
    spec = lambda a: pl.BlockSpec((a.shape[0] // STEPS, a.shape[1]), lambda i: (i, 0))
    outs = [jax.ShapeDtypeStruct(a.shape, a.dtype) for a in flat[3:]]
    new = pl.pallas_call(
        functools.partial(adamw_kernel, count),
        grid=(STEPS,),
        out_shape=outs,
        in_specs=[pl.BlockSpec(squares.shape, lambda i: (0, 0, 0))] + [spec(a) for a in flat],
        out_specs=[spec(a) for a in outs],
        compiler_params=pltpu.CompilerParams(vmem_limit_bytes=66_000_000),
        name="adamw",
    )(squares, *flat)
    return tuple(a.reshape(2, -1, a.shape[-1]) for a in new)


def solution(mesh):
    def step(x, dy, *arrays):
        weights, m, v = (arrays[i : i + 3] for i in (0, 3, 6))
        *gradients, squares = gradients_of(x[0], dy[0], *weights)
        return adamw(gradients, squares, mesh.shape["dp"] * sum(g.size for g in gradients), weights, m, v)

    states, cuts = P(("rep", "dp"), None, None), P(None, "dp", None)
    return jax.shard_map(
        step,
        mesh=mesh,
        in_specs=(states, states) + (cuts,) * 9,
        out_specs=(P("rep", "dp", None),) * 9,
        check_vma=NO,
    )
```
